32 devices in a mesh: slab: 4 (over y, x), sub: 8 (over z, core).
Axes of the slice: x: 2, y: 2, z: 4, core: 2. Of those that a mesh axis runs over, the one named last changes fastest.
Arguments:
- offsets: float32 [3, 4, 8, 64, 128], P(None, None, 'slab', 'sub'), may hold values from -0.5 to 0.5
- velocities: float32 [3, 4, 8, 64, 128], P(None, None, 'slab', 'sub'), may hold values from -6 to 6
- chain_label: int32 [4, 8, 64, 128], P(None, 'slab', 'sub'), may hold values from -1 to 31999, as said below
- partners: int32 [2, 4, 8, 64, 128], P(None, None, 'slab', 'sub'), may hold values from 16 to 91, as said below
- anchored: int32 [4, 8, 64, 128], P(None, 'slab', 'sub'), may hold values 0 or 1
Outputs:
- positions: float32 [3, 4, 8, 64, 128], P(None, None, 'slab', 'sub')
- half_velocity: float32 [3, 4, 8, 64, 128], P(None, None, 'slab', 'sub')
- unit_force: float32 [3, 4, 8, 64, 128], P(None, None, 'slab', 'sub')
The draws below stay inside these ranges and needn't reach their ends.
Inputs may be any that keep to these rules, and one draw needn't show every extreme that they name: `chain_label`: beads that carry equal labels within one cell's neighbourhood belong to one loop; -1 marks an empty slot. `partners`: the two codes of a bead name the previous and the next bead of its own loop, in a neighbouring cell, and that bead names it back; every loop is closed. The codes of an empty slot are its own code.
All inputs are finite; a program needn't handle non-finite values. No bound on the sum of `anchored` on one device may be relied on, other than what follows from the above.
Results may differ from the reference program's by a relative error of at most 0.0003.
Values sent between devices are 32-bit elements; how exact they have to be, the bound alone decides.
No kernel may reach another device: no remote copies, remote signals or barrier semaphores. Data moves between devices by JAX's collectives and lax.ppermute only.
A program may use at most 64 MiB of HBM per device.

```python
import jax
import jax.numpy as jnp
from jax import lax

SLOTS = 4
DESCENTS = 3
NZ = 128
NX = 8
NY = 64


def draw_offsets(key, part):
    column_x = jnp.arange(NX, dtype=jnp.float32)
    rising = (column_x + 0.5) / NX
    spread = 0.08 + 0.42 * rising
    uniform_base = jnp.clip(0.6 * jax.random.normal(key, (3, SLOTS, NX, NY, NZ), jnp.float32), -1.0, 1.0)
    return uniform_base * spread[None, None, :, None, None]


def loop_layout(key):
    key_first = jax.random.fold_in(key, 11)
    key_gap = jax.random.fold_in(key, 23)
    key_pick = jax.random.fold_in(key, 37)
    first_slot = jax.random.randint(key_first, (NX, NY, NZ), 0, SLOTS, dtype=jnp.int32)
    gap_slot = jax.random.randint(key_gap, (NX, NY, NZ), 1, SLOTS, dtype=jnp.int32)
    second_slot = (first_slot + gap_slot) % SLOTS
    pick = jax.random.randint(key_pick, (NX, NY, NZ), 0, 2, dtype=jnp.int32)
    slot_zero = jnp.where(pick == 0, first_slot, second_slot)
    slot_one = jnp.where(pick == 0, second_slot, first_slot)
    return (slot_zero, slot_one)


def cell_grid():
    grid_x = jnp.broadcast_to(jnp.arange(NX, dtype=jnp.int32)[:, None, None], (NX, NY, NZ))
    grid_y = jnp.broadcast_to(jnp.arange(NY, dtype=jnp.int32)[None, :, None], (NX, NY, NZ))
    grid_z = jnp.broadcast_to(jnp.arange(NZ, dtype=jnp.int32)[None, None, :], (NX, NY, NZ))
    return (grid_x, grid_y, grid_z)


def shifted_grid():
    grid_x, grid_y, grid_z = cell_grid()
    moved_x = (grid_x + (NX - 1)) % NX
    moved_y = (grid_y + (NY - 1)) % NY
    moved_z = (grid_z + (NZ - 1)) % NZ
    return (grid_x, grid_y, grid_z, moved_x, moved_y, moved_z)


def draw_chain_label(key, part):
    slot_zero, slot_one = loop_layout(key)
    grid_x, grid_y, grid_z, moved_x, moved_y, moved_z = shifted_grid()
    block_id = (moved_x // 2 * 7919 + moved_y // 2 * 104729 + moved_z // 4 * 1299) % 16000
    slot_ids = jnp.arange(SLOTS, dtype=jnp.int32)[:, None, None, None]
    label = jnp.where(slot_ids == slot_zero[None], block_id[None] * 2, jnp.where(slot_ids == slot_one[None], block_id[None] * 2 + 1, -1))
    return label.astype(jnp.int32)


def cycle_cell(place):
    quarter = place // 4
    remain = place % 4
    local_z = jnp.where(quarter % 2 == 0, remain, 3 - remain)
    local_x = jnp.where((quarter == 1) | (quarter == 2), 1, 0)
    local_y = jnp.where(quarter >= 2, 1, 0)
    return (local_x, local_y, local_z)


def draw_partners(key, part):
    slot_zero, slot_one = loop_layout(key)
    grid_x, grid_y, grid_z, moved_x, moved_y, moved_z = shifted_grid()
    local_x = moved_x % 2
    local_y = moved_y % 2
    local_z = moved_z % 4
    quarter = jnp.where(local_x == 0, jnp.where(local_y == 0, 0, 3), jnp.where(local_y == 0, 1, 2))
    place = quarter * 4 + jnp.where(quarter % 2 == 0, local_z, 3 - local_z)
    slot_ids = jnp.arange(SLOTS, dtype=jnp.int32)[:, None, None, None]
    codes = []
    for delta in (-1, 1):
        other_x, other_y, other_z = cycle_cell((place + delta) % 16)
        near_x = (grid_x - local_x + other_x + NX) % NX
        near_y = (grid_y - local_y + other_y + NY) % NY
        near_z = (grid_z - local_z + other_z + NZ) % NZ
        cell_code = 9 * (other_x - local_x + 1) + 3 * (other_y - local_y + 1) + (other_z - local_z + 1)
        near_zero = slot_zero[near_x, near_y, near_z]
        near_one = slot_one[near_x, near_y, near_z]
        code = jnp.where(slot_ids == slot_zero[None], cell_code[None] * SLOTS + near_zero[None], jnp.where(slot_ids == slot_one[None], cell_code[None] * SLOTS + near_one[None], 13 * SLOTS + slot_ids))
        codes.append(code)
    return jnp.stack(codes, axis=0).astype(jnp.int32)


def plant(entries, own_key, least, top_value):
    extent = entries.shape
    spot = [jax.random.randint(jax.random.fold_in(own_key, axis), (), 0, extent[axis]) for axis in range(len(extent))]
    entries = entries.at[tuple(spot)].set(least)
    longest = extent.index(max(extent))
    spot[longest] = (spot[longest] + 1) % extent[longest]
    return entries.at[tuple(spot)].set(top_value)


def block_scale(key, dims, cuts, low, largest):
    def one(position, blocks):
        heights = jax.random.uniform(jax.random.fold_in(jax.random.fold_in(key, 6), position), (blocks,), jnp.float32, low / len(cuts), largest / len(cuts))
        return jnp.repeat(jnp.exp(heights), dims[position] // blocks).reshape((-1,) + (1,) * (len(dims) - position - 1))

    loudness = one(*cuts[0])
    for cut in cuts[1:]:
        loudness = loudness * one(*cut)
    return loudness


def centred(stream_key, shape, width, bound, cuts=(), kind=jnp.bfloat16):
    values = jax.random.normal(stream_key, shape, jnp.float32) * width
    if len(cuts) > 0:
        values = block_scale(stream_key, shape, cuts, -0.22, 0.18) * values
    return jnp.clip(values, min=-bound, max=bound).astype(kind)


def setup_inputs(seed: int = 0) -> dict:
    arg_keys = jax.random.split(jax.random.key(seed), 6)
    return {
        "offsets": draw_offsets(jax.random.fold_in(arg_keys[5], 71), 0),
        "velocities": centred(arg_keys[1], (3, SLOTS, NX, NY, NZ), 1.0, 6.0, ((2, 4), (3, 8)), jnp.float32),
        "chain_label": draw_chain_label(jax.random.fold_in(arg_keys[5], 71), 0),
        "partners": draw_partners(jax.random.fold_in(arg_keys[5], 71), 0),
        "anchored": plant((jax.random.randint(arg_keys[4], (SLOTS, NX, NY, NZ), 0, 1000) < 4).astype(jnp.int32), jax.random.fold_in(arg_keys[4], 1), 0, 1),
    }


cell_width = 1.25
cutoff_sq = 2.0 ** (1.0 / 3.0)
soft_floor = 0.64
bond_stiff = 100.0
bond_inv_sq = 1.0 / 9.0
fene_floor = 0.2
time_step = 0.01
half_step = 0.005
half_step_sq = 5e-05
step_length = 0.1
tiny_eps = 1e-06

def pair_force(own_pos, own_label, partner_codes, fetch_pos, fetch_label, keep_chain):
    slot_count = own_pos.shape[1]
    slot_ids = jnp.arange(slot_count, dtype=jnp.int32)
    own_live = own_label >= 0
    summed = jnp.zeros(own_pos.shape, jnp.float32)
    for offset_x in (-1, 0, 1):
        for offset_y in (-1, 0, 1):
            for offset_z in (-1, 0, 1):
                code_base = ((offset_x + 1) * 9 + (offset_y + 1) * 3 + (offset_z + 1)) * slot_count
                other_pos = fetch_pos(offset_x, offset_y, offset_z)
                other_label = fetch_label(offset_x, offset_y, offset_z)
                cell_shift = jnp.array([offset_x, offset_y, offset_z], jnp.float32) * cell_width
                separation = own_pos[:, :, None] - other_pos[:, None] - cell_shift[:, None, None, None, None, None]
                dist_sq = lax.optimization_barrier(jnp.sum(separation * separation, axis=0))
                pair_live = own_live[:, None] & (other_label[None] >= 0)
                if offset_x == 0 and offset_y == 0 and (offset_z == 0):
                    pair_live = pair_live & (slot_ids[:, None, None, None, None] != slot_ids[None, :, None, None, None])
                bond_live = pair_live
                if not keep_chain:
                    pair_live = pair_live & (own_label[:, None] != other_label[None])
                wca_live = pair_live & (dist_sq < cutoff_sq)
                inv_two = 1.0 / jnp.maximum(dist_sq, soft_floor)
                inv_four = inv_two * inv_two
                inv_eight = inv_four * inv_four
                wca_coef = jnp.where(wca_live, 24.0 * (2.0 * inv_eight * inv_four * inv_two - inv_eight), 0.0)
                wanted = (code_base + slot_ids)[None, None, :, None, None, None]
                matches = lax.optimization_barrier(jnp.sum((partner_codes[:, :, None] == wanted).astype(jnp.float32), axis=0))
                fene_coef = -bond_stiff / jnp.maximum(1.0 - dist_sq * bond_inv_sq, fene_floor)
                pair_coef = wca_coef + jnp.where(bond_live, matches, 0.0) * fene_coef
                summed = summed + lax.optimization_barrier(jnp.sum(pair_coef[None] * separation, axis=2))
    return summed

def global_force(positions, labels, partner_codes, keep_chain):
    pos_pad = jnp.concatenate([positions[:, :, -1:], positions, positions[:, :, :1]], axis=2)
    lab_pad = jnp.concatenate([labels[:, -1:], labels, labels[:, :1]], axis=1)

    def plane(plane_index):

        def fetch_pos(offset_x, offset_y, offset_z):
            neighbour = lax.dynamic_slice_in_dim(pos_pad, plane_index + 1 + offset_x, 1, 2)
            return jnp.roll(neighbour, (-offset_y, -offset_z), axis=(3, 4))

        def fetch_label(offset_x, offset_y, offset_z):
            neighbour = lax.dynamic_slice_in_dim(lab_pad, plane_index + 1 + offset_x, 1, 1)
            return jnp.roll(neighbour, (-offset_y, -offset_z), axis=(2, 3))
        own_pos = lax.dynamic_slice_in_dim(positions, plane_index, 1, 2)
        own_label = lax.dynamic_slice_in_dim(labels, plane_index, 1, 1)
        own_codes = lax.dynamic_slice_in_dim(partner_codes, plane_index, 1, 2)
        return pair_force(own_pos, own_label, own_codes, fetch_pos, fetch_label, keep_chain)[:, :, 0]
    planes = lax.map(plane, jnp.arange(NX, dtype=jnp.int32))
    return jnp.moveaxis(planes, 0, 2)

def reference(offsets, velocities, chain_label, partners, anchored):
    free_mask = ((chain_label >= 0) & (anchored == 0)).astype(jnp.float32)
    force_now = global_force(offsets, chain_label, partners, True) * free_mask
    moving = free_mask * velocities
    positions = offsets + (time_step * moving + half_step_sq * force_now)
    half_velocity = moving + half_step * force_now
    inverse = jnp.float32(1.0)
    for descent in range(DESCENTS):
        force_now = global_force(positions, chain_label, partners, False) * free_mask
        peak_force = jnp.sqrt(jnp.max(lax.optimization_barrier(jnp.sum(force_now * force_now, axis=0))))
        inverse = 1.0 / (peak_force + tiny_eps)
        positions = positions + step_length * inverse * force_now
    return (positions, half_velocity, inverse * force_now)
```

```python
import jax
import jax.numpy as jnp
from jax import lax
from jax.experimental import pallas as pl
from jax.experimental.pallas import tpu as pltpu
from jax.sharding import PartitionSpec as P

DESCENTS = 3

cell_width = 1.25
cutoff_sq = 2.0 ** (1.0 / 3.0)
soft_floor = 0.64
bond_stiff = 100.0
fene_floor = 0.2
time_step = 0.01
half_step = 0.005
half_step_sq = 5e-05
step_length = 0.1
tiny_eps = 1e-06

force_scale = 48.0
bond_range_sq = 9.0
bond_unit = -bond_stiff * bond_range_sq / force_scale
code_low, code_high = 16, 91


def row_select(tile, row, index):
    rows = lax.broadcasted_iota(jnp.int32, tile.shape, 0)
    return jnp.where(rows == index, jnp.broadcast_to(row, tile.shape), tile)


def spread(main, low, high, shift_y, shift_z, store):
    rows, lanes = main.shape
    for step_y in (-1, 0, 1):
        tile = main
        if step_y == -1:
            tile = row_select(pltpu.roll(main, 1, 0), low, 0)
        elif step_y == 1:
            tile = row_select(pltpu.roll(main, rows - 1, 0), high, rows - 1)
        if shift_y and step_y:
            tile = tile + step_y * cell_width
        for step_z in (-1, 0, 1):
            moved = tile
            if step_z == -1:
                moved = pltpu.roll(tile, 1, 1)
            elif step_z == 1:
                moved = pltpu.roll(tile, lanes - 1, 1)
            if shift_z and step_z:
                moved = moved + step_z * cell_width
            store((step_y + 1) * 3 + step_z + 1, moved)


class Field:
    def __init__(self, refs, planes, channels, rows):
        self.own, self.low, self.high, self.down, self.up = refs
        self.planes, self.channels, self.rows = planes, channels, rows

    def plane(self, plane, channel):
        rows = self.rows
        if 1 <= plane <= self.planes:
            return (
                self.own[plane - 1, channel],
                self.low[plane - 1, pl.ds(channel, 1)],
                self.high[plane - 1, pl.ds(channel, 1)],
            )
        edge = self.down if plane == 0 else self.up
        base = self.channels * rows
        half = (edge.shape[0] - base) // 2
        return (
            edge[pl.ds(channel * rows, rows)],
            edge[pl.ds(base + channel, 1)],
            edge[pl.ds(base + half + channel, 1)],
        )


def pair_terms(own, other, floor):
    sep = [a - b for a, b in zip(own, other)]
    dist_sq = sep[0] * sep[0] + sep[1] * sep[1] + sep[2] * sep[2]
    inv = 1.0 / jnp.maximum(dist_sq, floor)
    inv_two = inv * inv
    coef = (inv_two * inv_two) * (inv_two * inv - 0.5)
    return sep, dist_sq, coef


def bond_coef(dist_sq, strength):
    return strength * (1.0 / jnp.maximum(bond_range_sq - dist_sq, bond_range_sq * fene_floor))


def cell_runs(slots):
    bond_from, bond_to = code_low // slots, code_high // slots + 1
    marks = sorted({0, 9, 18, 27, bond_from, bond_to})
    return [(a, b, a >= bond_from and b <= bond_to) for a, b in zip(marks, marks[1:])]


def sweep(slots, planes, own_tile, near, body):
    totals = []
    for plane in range(planes):
        own = [own_tile(plane, c) for c in range(3 * slots)]
        acc = [jnp.zeros_like(own[0]) for _ in range(3 * slots)]
        for first, last, bonded in cell_runs(slots):
            step_x = first // 9 - 1
            moved = [own[s] - step_x * cell_width for s in range(slots)] + own[slots:]

            def step(cell, acc, moved=moved, bonded=bonded, plane=plane):
                acc = list(acc)
                for s2 in range(slots):
                    other = [near[plane * 9 + cell, c * slots + s2] for c in range(3)]
                    for s1 in range(slots):
                        mine = [moved[c * slots + s1] for c in range(3)]
                        coef, sep = body(plane, cell, s1, s2, mine, other, bonded)
                        for c in range(3):
                            acc[c * slots + s1] = acc[c * slots + s1] + coef * sep[c]
                return tuple(acc)

            acc = lax.fori_loop(first, last, step, tuple(acc))
        totals.append(list(acc))
    return totals


def put_rows(low_ref, high_ref, plane, channel, tile):
    rows = tile.shape[0]
    low_ref[plane, pl.ds(channel, 1)] = tile[0:1]
    high_ref[plane, pl.ds(channel, 1)] = tile[rows - 1 : rows]


def prepare_kernel(pos_ref, label_ref, field_ref, low_ref, high_ref):
    slots, planes = label_ref.shape[0], label_ref.shape[1]
    for plane in range(planes):
        for c in range(3 * slots):
            tile = pos_ref[c // slots, c % slots, plane]
            field_ref[plane, c] = tile
            put_rows(low_ref, high_ref, plane, c, tile)
        for s in range(slots):
            tile = label_ref[s, plane].astype(jnp.float32)
            field_ref[plane, 3 * slots + s] = tile
            put_rows(low_ref, high_ref, plane, 3 * slots + s, tile)


def verlet_kernel(
    vel_ref, label_ref, partner_ref, anchor_ref, own, low, high, down, up,
    half_ref, next_ref, next_low, next_high, pair_ref, near, near_label,
):
    slots, planes, rows, _ = label_ref.shape
    field = Field((own, low, high, down, up), planes, 4 * slots, rows)
    for plane in range(planes + 2):
        for c in range(4 * slots):
            into = near if c < 3 * slots else near_label

            def store(k, tile, into=into, plane=plane, c=c % (3 * slots)):
                into[plane * 9 + k, c] = tile

            main, lo, hi = field.plane(plane, c)
            spread(main, lo, hi, c // slots == 1, c // slots == 2, store)

    def body(plane, cell, s1, s2, mine, other, bonded):
        sep, dist_sq, coef = pair_terms(mine, other, soft_floor)
        label = label_ref[s1, plane].astype(jnp.float32)
        other_label = near_label[plane * 9 + cell, s2]
        alive = other_label >= 0.0
        coef = jnp.where(alive & (dist_sq < cutoff_sq), coef, 0.0)
        free = (label_ref[s1, plane] >= 0) & (anchor_ref[s1, plane] == 0)
        pair = jnp.where(alive & (label != other_label) & free, cutoff_sq, 0.0)
        if bonded:
            code = cell * slots + s2
            strength = jnp.where(partner_ref[0, s1, plane] == code, bond_unit, 0.0)
            strength = strength + jnp.where(partner_ref[1, s1, plane] == code, bond_unit, 0.0)
            strength = jnp.where(free, strength, 0.0)
            pair = jnp.where(strength < 0.0, strength, pair)
            coef = coef + bond_coef(dist_sq, strength)
        pair_ref[plane * 27 + cell, s2 * slots + s1] = pair
        return coef, sep

    totals = sweep(slots, planes, lambda plane, c: own[plane, c], near, body)
    for plane in range(planes):
        for c in range(3 * slots):
            s = c % slots
            free = ((label_ref[s, plane] >= 0) & (anchor_ref[s, plane] == 0)).astype(jnp.float32)
            force = totals[plane][c] * (free * force_scale)
            moving = free * vel_ref[c // slots, s, plane]
            half_ref[c // slots, s, plane] = moving + half_step * force
            place = own[plane, c] + (time_step * moving + half_step_sq * force)
            next_ref[plane, c] = place
            put_rows(next_low, next_high, plane, c, place)


def inverse_peak(peaks):
    peak_force = jnp.sqrt(jnp.max(jnp.max(peaks[...], axis=0, keepdims=True), axis=1, keepdims=True))
    return 1.0 / (peak_force + tiny_eps)


def descent_kernel(slots, planes, rows, moves, *refs):
    pair_ref, refs = refs[0], refs[1:]
    field = Field(refs[:5], planes, 3 * slots, rows)
    refs = refs[5:]
    if moves:
        force = Field(refs[:5], planes, 3 * slots, rows)
        scale = step_length * inverse_peak(refs[5])
        refs = refs[6:]
        moved = Field(refs[:5], planes, 3 * slots, rows)
        refs = refs[5:]
        for now, old, by in zip(refs_of(moved), refs_of(field), refs_of(force)):
            now[...] = old[...] + scale.reshape((1,) * now.ndim) * by[...]
        field = moved
    force_ref, force_low, force_high, peak_ref, near = refs
    for plane in range(planes + 2):
        for c in range(3 * slots):

            def store(k, tile, plane=plane, c=c):
                near[plane * 9 + k, c] = tile

            main, lo, hi = field.plane(plane, c)
            spread(main, lo, hi, c // slots == 1, c // slots == 2, store)

    def body(plane, cell, s1, s2, mine, other, bonded):
        sep, dist_sq, coef = pair_terms(mine, other, soft_floor)
        pair = pair_ref[plane * 27 + cell, s2 * slots + s1]
        rest = bond_coef(dist_sq, jnp.minimum(pair, 0.0)) if bonded else 0.0
        return jnp.where(dist_sq < pair, coef, rest), sep

    totals = sweep(slots, planes, lambda plane, c: field.own[plane, c], near, body)
    peak = None
    for plane in range(planes):
        forces = [total * force_scale for total in totals[plane]]
        for c in range(3 * slots):
            force_ref[plane, c] = forces[c]
            put_rows(force_low, force_high, plane, c, forces[c])
        for s in range(slots):
            size = sum(forces[c * slots + s] * forces[c * slots + s] for c in range(3))
            peak = size if peak is None else jnp.maximum(peak, size)
    peak_ref[...] = jnp.broadcast_to(jnp.max(peak, axis=0, keepdims=True), peak_ref.shape)


def refs_of(field):
    return (field.own, field.low, field.high, field.down, field.up)


def finish_kernel(place_ref, force_ref, peaks_ref, pos_ref, unit_ref):
    slots, planes = pos_ref.shape[1], pos_ref.shape[2]
    inverse = inverse_peak(peaks_ref)
    scale = step_length * inverse
    for plane in range(planes):
        for c in range(3 * slots):
            force = force_ref[plane, c]
            unit_ref[c // slots, c % slots, plane] = inverse * force
            pos_ref[c // slots, c % slots, plane] = place_ref[plane, c] + scale * force


def ring(axis):
    count = lax.axis_size(axis)
    forward = [(i, (i + 1) % count) for i in range(count)]
    return forward, [(b, a) for a, b in forward]


def halo(own, first_rows, last_rows):
    planes, channels, rows, lanes = own.shape
    forward, backward = ring("sub")
    low = lax.ppermute(last_rows, "sub", forward)
    high = lax.ppermute(first_rows, "sub", backward)

    def packed(plane):
        return jnp.concatenate(
            [own[plane].reshape(channels * rows, lanes), low[plane], high[plane]], axis=0
        )

    forward, backward = ring("slab")
    down = lax.ppermute(packed(planes - 1), "slab", forward)
    up = lax.ppermute(packed(0), "slab", backward)
    return (own, low, high, down, up)


def call(kernel, outs, scratch=(), flops=0):
    return pl.pallas_call(
        kernel,
        out_shape=[jax.ShapeDtypeStruct(shape, jnp.float32) for shape in outs],
        scratch_shapes=[pltpu.VMEM(shape, jnp.float32) for shape in scratch],
        cost_estimate=pl.CostEstimate(flops=flops, bytes_accessed=4 << 20, transcendentals=0),
    )


def shards(offsets, velocities, chain_label, partners, anchored):
    _, slots, planes, rows, lanes = offsets.shape
    devices = lax.axis_size("slab") * lax.axis_size("sub")
    padded = 4 * slots
    flops = planes * 27 * slots * slots * rows * lanes * 30
    field = (planes, 3 * slots, rows, lanes)
    edge = (planes, padded, lanes)
    near = ((planes + 2) * 9, 3 * slots, rows, lanes)
    wide, first, last = call(prepare_kernel, [(planes, 4 * slots, rows, lanes), edge, edge])(
        offsets, chain_label
    )
    start = halo(wide, first, last)
    half_velocity, place, first, last, pair = call(
        verlet_kernel,
        [velocities.shape, field, edge, edge, (planes * 27, slots * slots, rows, lanes)],
        [near, ((planes + 2) * 9, slots, rows, lanes)],
        flops,
    )(velocities, chain_label, partners, anchored, *start)
    places = halo(place, first, last)
    forces, peaks = (), None
    for descent in range(DESCENTS):
        moves = descent > 0

        def kernel(*refs, moves=moves):
            descent_kernel(slots, planes, rows, moves, *refs)

        outs = [field, edge, edge, (devices, lanes)]
        extra = (*forces, peaks) if moves else ()
        moved = [x.shape for x in places] if moves else []
        results = call(kernel, moved + outs, [near], flops)(pair, *places, *extra)
        if moves:
            places, results = results[:5], results[5:]
        force, first, last, peak = results
        peaks = lax.all_to_all(peak, ("slab", "sub"), 0, 0, tiled=True)
        if descent + 1 < DESCENTS:
            forces = halo(force, first, last)
    positions, unit_force = call(finish_kernel, [offsets.shape, offsets.shape])(
        places[0], force, peaks
    )
    return (positions, half_velocity, unit_force)


def solution(mesh):
    return jax.shard_map(
        shards,
        mesh=mesh,
        in_specs=(
            P(None, None, "slab", "sub", None),
            P(None, None, "slab", "sub", None),
            P(None, "slab", "sub", None),
            P(None, None, "slab", "sub", None),
            P(None, "slab", "sub", None),
        ),
        out_specs=(
            P(None, None, "slab", "sub", None),
            P(None, None, "slab", "sub", None),
            P(None, None, "slab", "sub", None),
        ),
        check_vma=False,
    )
```

```python
import jax
import jax.numpy as jnp
from jax import lax
from jax.experimental import pallas as pl
from jax.experimental.pallas import tpu as pltpu
from jax.sharding import PartitionSpec as P

DESCENTS = 3

cell_width = 1.25
cutoff_sq = 2.0 ** (1.0 / 3.0)
soft_floor = 0.64
bond_stiff = 100.0
fene_floor = 0.2
time_step = 0.01
half_step = 0.005
half_step_sq = 5e-05
step_length = 0.1
tiny_eps = 1e-06

force_scale = 48.0
bond_range_sq = 9.0
bond_unit = -bond_stiff * bond_range_sq / force_scale
code_low, code_high = 16, 91

vmem_limit = 12 << 20


def row_select(tile, row, index):
    rows = lax.broadcasted_iota(jnp.int32, tile.shape, 0)
    return jnp.where(rows == index, jnp.broadcast_to(row, tile.shape), tile)


def spread(main, low, high, shift_y, shift_z, store):
    rows, lanes = main.shape
    for step_y in (-1, 0, 1):
        tile = main
        if step_y == -1:
            tile = row_select(pltpu.roll(main, 1, 0), low, 0)
        elif step_y == 1:
            tile = row_select(pltpu.roll(main, rows - 1, 0), high, rows - 1)
        if shift_y and step_y:
            tile = tile + step_y * cell_width
        for step_z in (-1, 0, 1):
            moved = tile
            if step_z == -1:
                moved = pltpu.roll(tile, 1, 1)
            elif step_z == 1:
                moved = pltpu.roll(tile, lanes - 1, 1)
            if shift_z and step_z:
                moved = moved + step_z * cell_width
            store((step_y + 1) * 3 + step_z + 1, moved)


class Field:
    def __init__(self, refs, planes, channels, rows):
        self.own, self.low, self.high, self.down, self.up = refs
        self.planes, self.channels, self.rows = planes, channels, rows

    def plane(self, plane, channel):
        rows = self.rows
        if 1 <= plane <= self.planes:
            return (
                self.own[plane - 1, channel],
                self.low[plane - 1, pl.ds(channel, 1)],
                self.high[plane - 1, pl.ds(channel, 1)],
            )
        edge = self.down if plane == 0 else self.up
        base = self.channels * rows
        half = (edge.shape[0] - base) // 2
        return (
            edge[pl.ds(channel * rows, rows)],
            edge[pl.ds(base + channel, 1)],
            edge[pl.ds(base + half + channel, 1)],
        )


def pair_terms(own, other, floor):
    sep = [a - b for a, b in zip(own, other)]
    dist_sq = sep[0] * sep[0] + sep[1] * sep[1] + sep[2] * sep[2]
    inv = 1.0 / jnp.maximum(dist_sq, floor)
    inv_two = inv * inv
    coef = (inv_two * inv_two) * (inv_two * inv - 0.5)
    return sep, dist_sq, coef


def bond_coef(dist_sq, strength):
    return strength * (1.0 / jnp.maximum(bond_range_sq - dist_sq, bond_range_sq * fene_floor))


def cell_runs(slots):
    bond_from, bond_to = code_low // slots, code_high // slots + 1
    marks = sorted({0, 9, 18, 27, bond_from, bond_to})
    return [(a, b, a >= bond_from and b <= bond_to) for a, b in zip(marks, marks[1:])]


def sweep(slots, planes, own_tile, near, body):
    totals = []
    for plane in range(planes):
        own = [own_tile(plane, c) for c in range(3 * slots)]
        acc = [jnp.zeros_like(own[0]) for _ in range(3 * slots)]
        for first, last, bonded in cell_runs(slots):
            step_x = first // 9 - 1
            moved = [own[s] - step_x * cell_width for s in range(slots)] + own[slots:]

            def step(cell, acc, moved=moved, bonded=bonded, plane=plane):
                acc = list(acc)
                for s2 in range(slots):
                    other = [near[plane * 9 + cell, c * slots + s2] for c in range(3)]
                    for s1 in range(slots):
                        mine = [moved[c * slots + s1] for c in range(3)]
                        coef, sep = body(plane, cell, s1, s2, mine, other, bonded)
                        for c in range(3):
                            acc[c * slots + s1] = acc[c * slots + s1] + coef * sep[c]
                return tuple(acc)

            acc = lax.fori_loop(first, last, step, tuple(acc))
        totals.append(list(acc))
    return totals


def put_rows(low_ref, high_ref, plane, channel, tile):
    rows = tile.shape[0]
    low_ref[plane, pl.ds(channel, 1)] = tile[0:1]
    high_ref[plane, pl.ds(channel, 1)] = tile[rows - 1 : rows]


def prepare_kernel(pos_ref, label_ref, field_ref, low_ref, high_ref):
    slots, planes = label_ref.shape[0], label_ref.shape[1]
    for plane in range(planes):
        for c in range(3 * slots):
            tile = pos_ref[c // slots, c % slots, plane]
            field_ref[plane, c] = tile
            put_rows(low_ref, high_ref, plane, c, tile)
        for s in range(slots):
            tile = label_ref[s, plane].astype(jnp.float32)
            field_ref[plane, 3 * slots + s] = tile
            put_rows(low_ref, high_ref, plane, 3 * slots + s, tile)


def verlet_kernel(
    vel_ref, label_ref, partner_ref, anchor_ref, own, low, high, down, up,
    half_ref, next_ref, next_low, next_high, pair_ref, near, near_label,
):
    slots, planes, rows, _ = label_ref.shape
    field = Field((own, low, high, down, up), planes, 4 * slots, rows)
    for plane in range(planes + 2):
        for c in range(4 * slots):
            into = near if c < 3 * slots else near_label

            def store(k, tile, into=into, plane=plane, c=c % (3 * slots)):
                into[plane * 9 + k, c] = tile

            main, lo, hi = field.plane(plane, c)
            spread(main, lo, hi, c // slots == 1, c // slots == 2, store)

    def body(plane, cell, s1, s2, mine, other, bonded):
        sep, dist_sq, coef = pair_terms(mine, other, soft_floor)
        label = label_ref[s1, plane].astype(jnp.float32)
        other_label = near_label[plane * 9 + cell, s2]
        alive = other_label >= 0.0
        coef = jnp.where(alive & (dist_sq < cutoff_sq), coef, 0.0)
        free = (label_ref[s1, plane] >= 0) & (anchor_ref[s1, plane] == 0)
        pair = jnp.where(alive & (label != other_label) & free, cutoff_sq, 0.0)
        if bonded:
            code = cell * slots + s2
            strength = jnp.where(partner_ref[0, s1, plane] == code, bond_unit, 0.0)
            strength = strength + jnp.where(partner_ref[1, s1, plane] == code, bond_unit, 0.0)
            strength = jnp.where(free, strength, 0.0)
            pair = jnp.where(strength < 0.0, strength, pair)
            coef = coef + bond_coef(dist_sq, strength)
        pair_ref[plane * 27 + cell, s2 * slots + s1] = pair
        return coef, sep

    totals = sweep(slots, planes, lambda plane, c: own[plane, c], near, body)
    for plane in range(planes):
        for c in range(3 * slots):
            s = c % slots
            free = ((label_ref[s, plane] >= 0) & (anchor_ref[s, plane] == 0)).astype(jnp.float32)
            force = totals[plane][c] * (free * force_scale)
            moving = free * vel_ref[c // slots, s, plane]
            half_ref[c // slots, s, plane] = moving + half_step * force
            place = own[plane, c] + (time_step * moving + half_step_sq * force)
            next_ref[plane, c] = place
            put_rows(next_low, next_high, plane, c, place)


def inverse_peak(peaks):
    peak_force = jnp.sqrt(jnp.max(jnp.max(peaks[...], axis=0, keepdims=True), axis=1, keepdims=True))
    return 1.0 / (peak_force + tiny_eps)


def descent_kernel(slots, planes, rows, moves, last, *refs):
    if last:
        moved_halo, refs = refs[-4:], refs[:-4]
    pair_ref, refs = refs[0], refs[1:]
    field = Field(refs[:5], planes, 3 * slots, rows)
    refs = refs[5:]
    if moves:
        force = Field(refs[:5], planes, 3 * slots, rows)
        scale = step_length * inverse_peak(refs[5])
        refs = refs[6:]
        if last:
            moved, refs = (refs[0], *moved_halo), refs[1:]
        else:
            moved, refs = refs[:5], refs[5:]
        moved = Field(moved, planes, 3 * slots, rows)
        for now, old, by in zip(refs_of(moved), refs_of(field), refs_of(force)):
            now[...] = old[...] + scale.reshape((1,) * now.ndim) * by[...]
        field = moved
    if last:
        force_ref, peak_ref, near = refs
    else:
        force_ref, force_low, force_high, peak_ref, near = refs
    for plane in range(planes + 2):
        for c in range(3 * slots):

            def store(k, tile, plane=plane, c=c):
                near[plane * 9 + k, c] = tile

            main, lo, hi = field.plane(plane, c)
            spread(main, lo, hi, c // slots == 1, c // slots == 2, store)

    def body(plane, cell, s1, s2, mine, other, bonded):
        sep, dist_sq, coef = pair_terms(mine, other, soft_floor)
        pair = pair_ref[plane * 27 + cell, s2 * slots + s1]
        rest = bond_coef(dist_sq, jnp.minimum(pair, 0.0)) if bonded else 0.0
        return jnp.where(dist_sq < pair, coef, rest), sep

    totals = sweep(slots, planes, lambda plane, c: field.own[plane, c], near, body)
    peak = None
    for plane in range(planes):
        forces = [total * force_scale for total in totals[plane]]
        for c in range(3 * slots):
            force_ref[plane, c] = forces[c]
            if not last:
                put_rows(force_low, force_high, plane, c, forces[c])
        for s in range(slots):
            size = sum(forces[c * slots + s] * forces[c * slots + s] for c in range(3))
            peak = size if peak is None else jnp.maximum(peak, size)
    peak_ref[...] = jnp.broadcast_to(jnp.max(peak, axis=0, keepdims=True), peak_ref.shape)


def refs_of(field):
    return (field.own, field.low, field.high, field.down, field.up)


def finish_kernel(place_ref, force_ref, peaks_ref, pos_ref, unit_ref):
    slots, planes = pos_ref.shape[1], pos_ref.shape[2]
    inverse = inverse_peak(peaks_ref)
    scale = step_length * inverse
    for plane in range(planes):
        for c in range(3 * slots):
            force = force_ref[plane, c]
            unit_ref[c // slots, c % slots, plane] = inverse * force
            pos_ref[c // slots, c % slots, plane] = place_ref[plane, c] + scale * force


def ring(axis):
    count = lax.axis_size(axis)
    forward = [(i, (i + 1) % count) for i in range(count)]
    return forward, [(b, a) for a, b in forward]


def halo(own, first_rows, last_rows):
    planes, channels, rows, lanes = own.shape
    forward, backward = ring("sub")
    low = lax.ppermute(last_rows, "sub", forward)
    high = lax.ppermute(first_rows, "sub", backward)

    def packed(plane):
        return jnp.concatenate(
            [own[plane].reshape(channels * rows, lanes), low[plane], high[plane]], axis=0
        )

    forward, backward = ring("slab")
    down = lax.ppermute(packed(planes - 1), "slab", forward)
    up = lax.ppermute(packed(0), "slab", backward)
    return (own, low, high, down, up)


def call(kernel, outs, scratch=(), flops=0):
    return pl.pallas_call(
        kernel,
        out_shape=[jax.ShapeDtypeStruct(shape, jnp.float32) for shape in outs],
        scratch_shapes=[pltpu.VMEM(shape, jnp.float32) for shape in scratch],
        compiler_params=pltpu.CompilerParams(vmem_limit_bytes=vmem_limit),
        cost_estimate=pl.CostEstimate(flops=flops, bytes_accessed=4 << 20, transcendentals=0),
    )


def shards(offsets, velocities, chain_label, partners, anchored):
    _, slots, planes, rows, lanes = offsets.shape
    devices = lax.axis_size("slab") * lax.axis_size("sub")
    padded = 4 * slots
    flops = planes * 27 * slots * slots * rows * lanes * 30
    field = (planes, 3 * slots, rows, lanes)
    edge = (planes, padded, lanes)
    near = ((planes + 2) * 9, 3 * slots, rows, lanes)
    wide, first, last = call(prepare_kernel, [(planes, 4 * slots, rows, lanes), edge, edge])(
        offsets, chain_label
    )
    start = halo(wide, first, last)
    half_velocity, place, first, last, pair = call(
        verlet_kernel,
        [velocities.shape, field, edge, edge, (planes * 27, slots * slots, rows, lanes)],
        [near, ((planes + 2) * 9, slots, rows, lanes)],
        flops,
    )(velocities, chain_label, partners, anchored, *start)
    places = halo(place, first, last)
    forces, peaks = (), None
    for descent in range(DESCENTS):
        moves = descent > 0
        final = moves and descent + 1 == DESCENTS

        def kernel(*refs, moves=moves, final=final):
            descent_kernel(slots, planes, rows, moves, final, *refs)

        peak_shape = (devices, lanes)
        outs = [field, peak_shape] if final else [field, edge, edge, peak_shape]
        extra = (*forces, peaks) if moves else ()
        moved = [x.shape for x in places] if moves else []
        scratch = [near]
        if final:
            moved, scratch = moved[:1], scratch + moved[1:]
        results = call(kernel, moved + outs, scratch, flops)(pair, *places, *extra)
        if final:
            place, force, peak = results
        else:
            if moves:
                places, results = results[:5], results[5:]
            force, first, last, peak = results
        peaks = lax.all_to_all(peak, ("slab", "sub"), 0, 0, tiled=True)
        if not final:
            forces = halo(force, first, last)
    positions, unit_force = call(finish_kernel, [offsets.shape, offsets.shape])(
        place, force, peaks
    )
    return (positions, half_velocity, unit_force)


def solution(mesh):
    return jax.shard_map(
        shards,
        mesh=mesh,
        in_specs=(
            P(None, None, "slab", "sub", None),
            P(None, None, "slab", "sub", None),
            P(None, "slab", "sub", None),
            P(None, None, "slab", "sub", None),
            P(None, "slab", "sub", None),
        ),
        out_specs=(
            P(None, None, "slab", "sub", None),
            P(None, None, "slab", "sub", None),
            P(None, None, "slab", "sub", None),
        ),
        check_vma=False,
    )
```

```python
import jax
import jax.numpy as jnp
from jax import lax
from jax.experimental import pallas as pl
from jax.experimental.pallas import tpu as pltpu
from jax.sharding import PartitionSpec as P

DESCENTS = 3

cell_width = 1.25
soft_floor = 0.64
bond_stiff = 100.0
fene_floor = 0.2
time_step = 0.01
half_step = 0.005
half_step_sq = 5e-05
step_length = 0.1
tiny_eps = 1e-06

force_scale = 48.0
bond_range_sq = 9.0
live_barrier = 0.5
dead_barrier = 4.0
bond_unit = -bond_stiff * bond_range_sq / force_scale
code_low, code_high = 16, 91

vmem_limit = 12 << 20


def row_select(tile, row, index):
    rows = lax.broadcasted_iota(jnp.int32, tile.shape, 0)
    return jnp.where(rows == index, jnp.broadcast_to(row, tile.shape), tile)


def spread(main, low, high, shift_y, shift_z, store):
    rows, lanes = main.shape
    for step_y in (-1, 0, 1):
        tile = main
        if step_y == -1:
            tile = row_select(pltpu.roll(main, 1, 0), low, 0)
        elif step_y == 1:
            tile = row_select(pltpu.roll(main, rows - 1, 0), high, rows - 1)
        if shift_y and step_y:
            tile = tile + step_y * cell_width
        for step_z in (-1, 0, 1):
            moved = tile
            if step_z == -1:
                moved = pltpu.roll(tile, 1, 1)
            elif step_z == 1:
                moved = pltpu.roll(tile, lanes - 1, 1)
            if shift_z and step_z:
                moved = moved + step_z * cell_width
            store((step_y + 1) * 3 + step_z + 1, moved)


class Field:
    def __init__(self, refs, planes, channels, rows):
        self.own, self.low, self.high, self.down, self.up = refs
        self.planes, self.channels, self.rows = planes, channels, rows

    def plane(self, plane, channel):
        rows = self.rows
        if 1 <= plane <= self.planes:
            return (
                self.own[plane - 1, channel],
                self.low[plane - 1, pl.ds(channel, 1)],
                self.high[plane - 1, pl.ds(channel, 1)],
            )
        edge = self.down if plane == 0 else self.up
        base = self.channels * rows
        half = (edge.shape[0] - base) // 2
        return (
            edge[pl.ds(channel * rows, rows)],
            edge[pl.ds(base + channel, 1)],
            edge[pl.ds(base + half + channel, 1)],
        )


def pair_terms(own, other, barrier):
    sep = [a - b for a, b in zip(own, other)]
    dist_sq = sep[0] * sep[0] + sep[1] * sep[1] + sep[2] * sep[2]
    inv = 1.0 / jnp.maximum(dist_sq, soft_floor)
    inv_two = inv * inv
    coef = (inv_two * inv_two) * jnp.maximum(inv_two * inv - barrier, 0.0)
    return sep, dist_sq, coef


def bond_coef(dist_sq, strength):
    return strength * (1.0 / jnp.maximum(bond_range_sq - dist_sq, bond_range_sq * fene_floor))


def bond_cells(slots):
    return code_low // slots, code_high // slots + 1


def cell_runs(slots):
    bond_from, bond_to = bond_cells(slots)
    marks = sorted({0, 9, 18, 27, bond_from, bond_to})
    return [(a, b, a >= bond_from and b <= bond_to) for a, b in zip(marks, marks[1:])]


def sweep(slots, planes, own_tile, near, body):
    totals = []
    for plane in range(planes):
        own = [own_tile(plane, c) for c in range(3 * slots)]
        acc = [jnp.zeros_like(own[0]) for _ in range(3 * slots)]
        for first, last, bonded in cell_runs(slots):
            step_x = first // 9 - 1
            moved = [own[s] - step_x * cell_width for s in range(slots)] + own[slots:]

            def step(cell, acc, moved=moved, bonded=bonded, plane=plane):
                acc = list(acc)
                for s2 in range(slots):
                    other = [near[plane * 9 + cell, c * slots + s2] for c in range(3)]
                    each = body(plane, cell, s2, other, bonded)
                    for s1 in range(slots):
                        coef, sep = each(s1, [moved[c * slots + s1] for c in range(3)])
                        for c in range(3):
                            acc[c * slots + s1] = acc[c * slots + s1] + coef * sep[c]
                return tuple(acc)

            acc = lax.fori_loop(first, last, step, tuple(acc))
        totals.append(list(acc))
    return totals


def put_rows(low_ref, high_ref, plane, channel, tile):
    rows = tile.shape[0]
    low_ref[plane, pl.ds(channel, 1)] = tile[0:1]
    high_ref[plane, pl.ds(channel, 1)] = tile[rows - 1 : rows]


def prepare_kernel(wide_ref, field_ref, low_ref, high_ref):
    channels, planes, _, _ = wide_ref.shape
    for plane in range(planes):
        for c in range(channels):
            tile = wide_ref[c, plane]
            field_ref[plane, c] = tile
            put_rows(low_ref, high_ref, plane, c, tile)


def verlet_kernel(
    extra_ref, own, low, high, down, up,
    half_ref, next_ref, next_low, next_high, barrier_ref, bond_ref, weight_ref, near,
):
    _, slots, planes, rows, _ = half_ref.shape
    vel_at, partner_at, anchor_at = 0, 3 * slots, 5 * slots
    field = Field((own, low, high, down, up), planes, 4 * slots, rows)
    for plane in range(planes + 2):
        for c in range(4 * slots):

            def store(k, tile, plane=plane, c=c):
                near[plane * 9 + k, c] = tile

            main, lo, hi = field.plane(plane, c)
            spread(main, lo, hi, c // slots == 1, c // slots == 2, store)
    bond_from, bond_to = bond_cells(slots)

    def body(plane, cell, s2, other, bonded):
        label = near[plane * 9 + cell, 3 * slots + s2]
        alive = jnp.where(label < 0.0, dead_barrier, live_barrier)

        def each(s1, mine):
            sep, dist_sq, coef = pair_terms(mine, other, alive)
            barrier_ref[plane * 27 + cell, s2 * slots + s1] = jnp.where(
                label == own[plane, 3 * slots + s1], dead_barrier, alive
            )
            if bonded:
                code = (cell * slots + s2).astype(jnp.float32)
                strength = jnp.where(extra_ref[partner_at + s1, plane] == code, bond_unit, 0.0)
                strength += jnp.where(extra_ref[partner_at + slots + s1, plane] == code, bond_unit, 0.0)
                bond_ref[plane * (bond_to - bond_from) + cell - bond_from, s2 * slots + s1] = strength
                coef += bond_coef(dist_sq, strength)
            return coef, sep

        return each

    totals = sweep(slots, planes, lambda plane, c: own[plane, c], near, body)
    for plane in range(planes):
        for s in range(slots):
            free = ((own[plane, 3 * slots + s] >= 0.0) & (extra_ref[anchor_at + s, plane] == 0.0)).astype(jnp.float32)
            weight_ref[plane, s] = free * force_scale
            for c in range(s, 3 * slots, slots):
                force = totals[plane][c] * (free * force_scale)
                moving = free * extra_ref[vel_at + c, plane]
                half_ref[c // slots, s, plane] = moving + half_step * force
                place = own[plane, c] + (time_step * moving + half_step_sq * force)
                next_ref[plane, c] = place
                put_rows(next_low, next_high, plane, c, place)


def inverse_peak(peaks):
    peak_force = jnp.sqrt(jnp.max(jnp.max(peaks[...], axis=0, keepdims=True), axis=1, keepdims=True))
    return 1.0 / (peak_force + tiny_eps)


def descent_kernel(slots, planes, rows, moves, last, *refs):
    if last:
        moved_halo, refs = refs[-4:], refs[:-4]
    (barrier_ref, bond_ref, weight_ref), refs = refs[:3], refs[3:]
    field = Field(refs[:5], planes, 3 * slots, rows)
    refs = refs[5:]
    if moves:
        force = Field(refs[:5], planes, 3 * slots, rows)
        scale = step_length * inverse_peak(refs[5])
        refs = refs[6:]
        if last:
            moved, refs = (refs[0], *moved_halo), refs[1:]
        else:
            moved, refs = refs[:5], refs[5:]
        moved = Field(moved, planes, 3 * slots, rows)
        for now, old, by in zip(refs_of(moved), refs_of(field), refs_of(force)):
            now[...] = old[...] + scale.reshape((1,) * now.ndim) * by[...]
        field = moved
    if last:
        force_ref, peak_ref, near = refs
    else:
        force_ref, force_low, force_high, peak_ref, near = refs
    for plane in range(planes + 2):
        for c in range(3 * slots):

            def store(k, tile, plane=plane, c=c):
                near[plane * 9 + k, c] = tile

            main, lo, hi = field.plane(plane, c)
            spread(main, lo, hi, c // slots == 1, c // slots == 2, store)

    bond_from, bond_to = bond_cells(slots)

    def body(plane, cell, s2, other, bonded):
        def each(s1, mine):
            k = s2 * slots + s1
            sep, dist_sq, coef = pair_terms(mine, other, barrier_ref[plane * 27 + cell, k])
            if bonded:
                coef += bond_coef(dist_sq, bond_ref[plane * (bond_to - bond_from) + cell - bond_from, k])
            return coef, sep

        return each

    totals = sweep(slots, planes, lambda plane, c: field.own[plane, c], near, body)
    peak = None
    for plane in range(planes):
        forces = [total * weight_ref[plane, c % slots] for c, total in enumerate(totals[plane])]
        for c in range(3 * slots):
            force_ref[plane, c] = forces[c]
            if not last:
                put_rows(force_low, force_high, plane, c, forces[c])
        for s in range(slots):
            size = sum(forces[c * slots + s] * forces[c * slots + s] for c in range(3))
            peak = size if peak is None else jnp.maximum(peak, size)
    peak_ref[...] = jnp.broadcast_to(jnp.max(peak, axis=0, keepdims=True), peak_ref.shape)


def refs_of(field):
    return (field.own, field.low, field.high, field.down, field.up)


def finish_kernel(place_ref, force_ref, peaks_ref, pos_ref, unit_ref):
    slots, planes = pos_ref.shape[1], pos_ref.shape[2]
    inverse = inverse_peak(peaks_ref)
    scale = step_length * inverse
    for plane in range(planes):
        for c in range(3 * slots):
            force = force_ref[plane, c]
            unit_ref[c // slots, c % slots, plane] = inverse * force
            pos_ref[c // slots, c % slots, plane] = place_ref[plane, c] + scale * force


def ring(axis):
    count = lax.axis_size(axis)
    forward = [(i, (i + 1) % count) for i in range(count)]
    return forward, [(b, a) for a, b in forward]


def halo(own, first_rows, last_rows):
    planes, channels, rows, lanes = own.shape
    forward, backward = ring("sub")
    low = lax.ppermute(last_rows, "sub", forward)
    high = lax.ppermute(first_rows, "sub", backward)

    def packed(plane):
        return jnp.concatenate(
            [own[plane].reshape(channels * rows, lanes), low[plane], high[plane]], axis=0
        )

    forward, backward = ring("slab")
    down = lax.ppermute(packed(planes - 1), "slab", forward)
    up = lax.ppermute(packed(0), "slab", backward)
    return (own, low, high, down, up)


def call(kernel, outs, scratch=(), flops=0):
    return pl.pallas_call(
        kernel,
        out_shape=[jax.ShapeDtypeStruct(shape, jnp.float32) for shape in outs],
        scratch_shapes=[pltpu.VMEM(shape, jnp.float32) for shape in scratch],
        compiler_params=pltpu.CompilerParams(vmem_limit_bytes=vmem_limit),
        cost_estimate=pl.CostEstimate(flops=flops, bytes_accessed=4 << 20, transcendentals=0),
    )


def shards(offsets, velocities, chain_label, partners, anchored):
    _, slots, planes, rows, lanes = offsets.shape
    devices = lax.axis_size("slab") * lax.axis_size("sub")
    padded = 4 * slots
    flops = planes * 27 * slots * slots * rows * lanes * 30
    tiles = (rows, lanes)
    field = (planes, 3 * slots, *tiles)
    edge = (planes, padded, lanes)
    near = ((planes + 2) * 9, 3 * slots, *tiles)
    bond_from, bond_to = bond_cells(slots)
    pairs = [
        (planes * 27, slots * slots, *tiles),
        (planes * (bond_to - bond_from), slots * slots, *tiles),
        (planes, slots, *tiles),
    ]
    flat = offsets.reshape(3 * slots, planes, *tiles)
    labels = chain_label.astype(jnp.float32)
    wide = jnp.concatenate([flat, labels], axis=0)
    start = halo(*call(prepare_kernel, [(planes, 4 * slots, *tiles), edge, edge])(wide))
    extra = jnp.concatenate(
        [
            velocities.reshape(3 * slots, planes, *tiles),
            partners.reshape(2 * slots, planes, *tiles).astype(jnp.float32),
            anchored.astype(jnp.float32),
        ],
        axis=0,
    )
    half_velocity, place, first, last, *pairs = call(
        verlet_kernel,
        [velocities.shape, field, edge, edge, *pairs],
        [((planes + 2) * 9, 4 * slots, *tiles)],
        flops,
    )(extra, *start)
    places = halo(place, first, last)
    forces, peaks = (), None
    for descent in range(DESCENTS):
        moves = descent > 0
        final = moves and descent + 1 == DESCENTS

        def kernel(*refs, moves=moves, final=final):
            descent_kernel(slots, planes, rows, moves, final, *refs)

        peak_shape = (devices, lanes)
        outs = [field, peak_shape] if final else [field, edge, edge, peak_shape]
        extra = (*forces, peaks) if moves else ()
        moved = [x.shape for x in places] if moves else []
        scratch = [near]
        if final:
            moved, scratch = moved[:1], scratch + moved[1:]
        results = call(kernel, moved + outs, scratch, flops)(*pairs, *places, *extra)
        if final:
            place, force, peak = results
        else:
            if moves:
                places, results = results[:5], results[5:]
            force, first, last, peak = results
        peaks = lax.all_to_all(peak, ("slab", "sub"), 0, 0, tiled=True)
        if not final:
            forces = halo(force, first, last)
    positions, unit_force = call(finish_kernel, [offsets.shape, offsets.shape])(
        place, force, peaks
    )
    return (positions, half_velocity, unit_force)


def solution(mesh):
    return jax.shard_map(
        shards,
        mesh=mesh,
        in_specs=(
            P(None, None, "slab", "sub", None),
            P(None, None, "slab", "sub", None),
            P(None, "slab", "sub", None),
            P(None, None, "slab", "sub", None),
            P(None, "slab", "sub", None),
        ),
        out_specs=(
            P(None, None, "slab", "sub", None),
            P(None, None, "slab", "sub", None),
            P(None, None, "slab", "sub", None),
        ),
        check_vma=False,
    )
```

```python
import jax
import jax.numpy as jnp
from jax import lax
from jax.experimental import pallas as pl
from jax.experimental.pallas import tpu as pltpu
from jax.sharding import PartitionSpec as P

DESCENTS = 3

cell_width = 1.25
soft_floor = 0.64
bond_stiff = 100.0
fene_floor = 0.2
time_step = 0.01
half_step = 0.005
half_step_sq = 5e-05
step_length = 0.1
tiny_eps = 1e-06

force_scale = 48.0
bond_range_sq = 9.0
live_barrier = 0.5
dead_barrier = 4.0
bond_unit = -bond_stiff * bond_range_sq / force_scale
code_low, code_high = 16, 91

vmem_limit = 12 << 20


def row_select(tile, row, index):
    rows = lax.broadcasted_iota(jnp.int32, tile.shape, 0)
    return jnp.where(rows == index, jnp.broadcast_to(row, tile.shape), tile)


def spread(main, low, high, shift_y, shift_z, store):
    rows, lanes = main.shape
    for step_y in (-1, 0, 1):
        tile = main
        if step_y == -1:
            tile = row_select(pltpu.roll(main, 1, 0), low, 0)
        elif step_y == 1:
            tile = row_select(pltpu.roll(main, rows - 1, 0), high, rows - 1)
        if shift_y and step_y:
            tile = tile + step_y * cell_width
        for step_z in (-1, 0, 1):
            moved = tile
            if step_z == -1:
                moved = pltpu.roll(tile, 1, 1)
            elif step_z == 1:
                moved = pltpu.roll(tile, lanes - 1, 1)
            if shift_z and step_z:
                moved = moved + step_z * cell_width
            store((step_y + 1) * 3 + step_z + 1, moved)


class Field:
    def __init__(self, refs, planes, channels, rows):
        self.own, self.low, self.high, self.down, self.up = refs
        self.planes, self.channels, self.rows = planes, channels, rows

    def plane(self, plane, channel):
        rows = self.rows
        if 1 <= plane <= self.planes:
            return (
                self.own[plane - 1, channel],
                self.low[plane - 1, pl.ds(channel, 1)],
                self.high[plane - 1, pl.ds(channel, 1)],
            )
        edge = self.down if plane == 0 else self.up
        base = self.channels * rows
        half = (edge.shape[0] - base) // 2
        return (
            edge[pl.ds(channel * rows, rows)],
            edge[pl.ds(base + channel, 1)],
            edge[pl.ds(base + half + channel, 1)],
        )


def pair_terms(own, other, barrier):
    sep = [a - b for a, b in zip(own, other)]
    dist_sq = sep[0] * sep[0] + sep[1] * sep[1] + sep[2] * sep[2]
    inv = 1.0 / jnp.maximum(dist_sq, soft_floor)
    inv_two = inv * inv
    coef = (inv_two * inv_two) * jnp.maximum(inv_two * inv - barrier, 0.0)
    return sep, dist_sq, coef


def bond_coef(dist_sq, strength):
    return strength * (1.0 / jnp.maximum(bond_range_sq - dist_sq, bond_range_sq * fene_floor))


def bond_cells(slots):
    return code_low // slots, code_high // slots + 1


def cell_runs(slots):
    bond_from, bond_to = bond_cells(slots)
    marks = sorted({0, 9, 18, 27, bond_from, bond_to})
    return [(a, b, a >= bond_from and b <= bond_to) for a, b in zip(marks, marks[1:])]


def sweep(slots, planes, own_tile, near, body):
    totals = []
    for plane in range(planes):
        own = [own_tile(plane, c) for c in range(3 * slots)]
        acc = [jnp.zeros_like(own[0]) for _ in range(3 * slots)]
        for first, last, bonded in cell_runs(slots):
            step_x = first // 9 - 1
            moved = [own[s] - step_x * cell_width for s in range(slots)] + own[slots:]

            def step(cell, acc, moved=moved, bonded=bonded, plane=plane):
                acc = list(acc)
                for s2 in range(slots):
                    other = [near[plane * 9 + cell, c * slots + s2] for c in range(3)]
                    each = body(plane, cell, s2, other, bonded)
                    for s1 in range(slots):
                        coef, sep = each(s1, [moved[c * slots + s1] for c in range(3)])
                        for c in range(3):
                            acc[c * slots + s1] = acc[c * slots + s1] + coef * sep[c]
                return tuple(acc)

            acc = lax.fori_loop(first, last, step, tuple(acc))
        totals.append(list(acc))
    return totals


def put_rows(low_ref, high_ref, plane, channel, tile):
    rows = tile.shape[0]
    low_ref[plane, pl.ds(channel, 1)] = tile[0:1]
    high_ref[plane, pl.ds(channel, 1)] = tile[rows - 1 : rows]


def prepare_kernel(wide_ref, field_ref, low_ref, high_ref):
    channels, planes, _, _ = wide_ref.shape
    for plane in range(planes):
        for c in range(channels):
            tile = wide_ref[c, plane]
            field_ref[plane, c] = tile
            put_rows(low_ref, high_ref, plane, c, tile)


def verlet_kernel(
    extra_ref, own, low, high, down, up,
    half_ref, next_ref, next_low, next_high, barrier_ref, weight_ref, near,
):
    _, slots, planes, rows, _ = half_ref.shape
    vel_at, partner_at, anchor_at = 0, 3 * slots, 5 * slots
    field = Field((own, low, high, down, up), planes, 4 * slots, rows)
    for plane in range(planes + 2):
        for c in range(4 * slots):

            def store(k, tile, plane=plane, c=c):
                near[plane * 9 + k, c] = tile

            main, lo, hi = field.plane(plane, c)
            spread(main, lo, hi, c // slots == 1, c // slots == 2, store)

    def body(plane, cell, s2, other, bonded):
        label = near[plane * 9 + cell, 3 * slots + s2]
        alive = jnp.where(label < 0.0, dead_barrier, live_barrier)

        def each(s1, mine):
            sep, dist_sq, coef = pair_terms(mine, other, alive)
            barrier = jnp.where(label == own[plane, 3 * slots + s1], dead_barrier, alive)
            if bonded:
                code = (cell * slots + s2).astype(jnp.float32)
                strength = jnp.where(extra_ref[partner_at + s1, plane] == code, bond_unit, 0.0)
                strength += jnp.where(extra_ref[partner_at + slots + s1, plane] == code, bond_unit, 0.0)
                barrier = jnp.where(strength < 0.0, dead_barrier - strength, barrier)
                coef += bond_coef(dist_sq, strength)
            pending.append(barrier)
            if len(pending) == 2:
                both = jnp.concatenate(pending, axis=0).astype(barrier_ref.dtype)
                barrier_ref[plane * 27 + cell, (s2 * slots + s1) // 2] = both
                pending.clear()
            return coef, sep

        return each

    pending = []
    totals = sweep(slots, planes, lambda plane, c: own[plane, c], near, body)
    for plane in range(planes):
        for s in range(slots):
            free = ((own[plane, 3 * slots + s] >= 0.0) & (extra_ref[anchor_at + s, plane] == 0.0)).astype(jnp.float32)
            weight_ref[plane, s] = free * force_scale
            for c in range(s, 3 * slots, slots):
                force = totals[plane][c] * (free * force_scale)
                moving = free * extra_ref[vel_at + c, plane]
                half_ref[c // slots, s, plane] = moving + half_step * force
                place = own[plane, c] + (time_step * moving + half_step_sq * force)
                next_ref[plane, c] = place
                put_rows(next_low, next_high, plane, c, place)


def inverse_peak(peaks):
    peak_force = jnp.sqrt(jnp.max(jnp.max(peaks, axis=0, keepdims=True), axis=1, keepdims=True))
    return 1.0 / (peak_force + tiny_eps)


def descent_kernel(slots, planes, rows, moves, last, *refs):
    refs = list(refs)

    def take(count):
        taken = refs[:count]
        del refs[:count]
        return taken

    ids, barrier_ref, weight_ref = take(3)
    places = take(5)
    if moves:
        own, low, high, down, up, mixed = take(6)
        now = take(1) + refs[-4:] if last else take(5)
        if last:
            del refs[-4:]
        scale = step_length * inverse_peak(mixed[:, mixed.shape[1] - 1, :])
        for i, by in enumerate((own, low, high)):
            now[i][...] = places[i][...] + scale.reshape((1,) * len(by.shape)) * by[...]
        for i, by, corners in ((3, down, (3, 2)), (4, up, (1, 0))):
            base, pad = by.shape[0], mixed.shape[1]
            now[i][pl.ds(0, base)] = places[i][pl.ds(0, base)] + scale * by[...]
            for side, corner in enumerate(corners):
                at = pl.ds(base + side * pad, pad)
                now[i][at] = places[i][at] + scale * mixed[ids[corner]]
        places = now
    field = Field(places, planes, 3 * slots, rows)
    if last:
        force_ref, peak_ref, near = refs
    else:
        force_ref, force_low, force_high, mix_ref, near = refs
    for plane in range(planes + 2):
        for c in range(3 * slots):

            def store(k, tile, plane=plane, c=c):
                near[plane * 9 + k, c] = tile

            main, lo, hi = field.plane(plane, c)
            spread(main, lo, hi, c // slots == 1, c // slots == 2, store)

    def body(plane, cell, s2, other, bonded):
        both = [
            barrier_ref[plane * 27 + cell, (s2 * slots) // 2 + i].astype(jnp.float32)
            for i in range(slots // 2)
        ]

        def each(s1, mine):
            barrier = both[s1 // 2][(s1 % 2) * rows : (s1 % 2 + 1) * rows]
            sep, dist_sq, coef = pair_terms(mine, other, barrier)
            if bonded:
                coef += bond_coef(dist_sq, jnp.minimum(dead_barrier - barrier, 0.0))
            return coef, sep

        return each

    totals = sweep(slots, planes, lambda plane, c: field.own[plane, c], near, body)
    peak = None
    for plane in range(planes):
        forces = [total * weight_ref[plane, c % slots] for c, total in enumerate(totals[plane])]
        for c in range(3 * slots):
            force_ref[plane, c] = forces[c]
            if not last:
                put_rows(force_low, force_high, plane, c, forces[c])
        for s in range(slots):
            size = sum(forces[c * slots + s] * forces[c * slots + s] for c in range(3))
            peak = size if peak is None else jnp.maximum(peak, size)
    peak = jnp.max(peak, axis=0, keepdims=True)
    if last:
        peak_ref[...] = jnp.broadcast_to(peak, peak_ref.shape)
        return

    def fill(device, carry):
        mix_ref[device] = jnp.broadcast_to(peak, mix_ref.shape[1:])
        return carry

    lax.fori_loop(0, mix_ref.shape[0], fill, 0)
    for corner in range(4):
        plane = planes - 1 if corner < 2 else 0
        rows_ref = force_high if corner % 2 == 0 else force_low
        mix_ref[ids[corner], pl.ds(0, 3 * slots)] = rows_ref[plane, pl.ds(0, 3 * slots)]


def finish_kernel(place_ref, force_ref, peaks_ref, pos_ref, unit_ref):
    slots, planes = pos_ref.shape[1], pos_ref.shape[2]
    inverse = inverse_peak(peaks_ref[...])
    scale = step_length * inverse
    for plane in range(planes):
        for c in range(3 * slots):
            force = force_ref[plane, c]
            unit_ref[c // slots, c % slots, plane] = inverse * force
            pos_ref[c // slots, c % slots, plane] = place_ref[plane, c] + scale * force


def ring(axis):
    count = lax.axis_size(axis)
    forward = [(i, (i + 1) % count) for i in range(count)]
    return forward, [(b, a) for a, b in forward]


def halo(own, first_rows, last_rows):
    planes, channels, rows, lanes = own.shape
    forward, backward = ring("sub")
    low = lax.ppermute(last_rows, "sub", forward)
    high = lax.ppermute(first_rows, "sub", backward)

    def packed(plane):
        return jnp.concatenate(
            [own[plane].reshape(channels * rows, lanes), low[plane], high[plane]], axis=0
        )

    forward, backward = ring("slab")
    down = lax.ppermute(packed(planes - 1), "slab", forward)
    up = lax.ppermute(packed(0), "slab", backward)
    return (own, low, high, down, up)


def near_halo(own, first_rows, last_rows):
    planes, channels, rows, lanes = own.shape
    forward, backward = ring("sub")
    low = lax.ppermute(last_rows, "sub", forward)
    high = lax.ppermute(first_rows, "sub", backward)
    forward, backward = ring("slab")
    flat = (channels * rows, lanes)
    down = lax.ppermute(own[planes - 1].reshape(flat), "slab", forward)
    up = lax.ppermute(own[0].reshape(flat), "slab", backward)
    return (own, low, high, down, up)


def corner_devices():
    slabs, subs = lax.axis_size("slab"), lax.axis_size("sub")
    x, y = lax.axis_index("slab"), lax.axis_index("sub")
    return jnp.stack(
        [
            ((x + i + slabs) % slabs) * subs + (y + j + subs) % subs
            for i in (1, -1)
            for j in (1, -1)
        ]
    ).astype(jnp.int32)


def call(kernel, outs, scratch=(), flops=0, scalars=0, inputs=0):
    specs = {}
    if scalars:
        specs["in_specs"] = [pl.BlockSpec(memory_space=pltpu.SMEM)] * scalars
        specs["in_specs"] += [pl.BlockSpec(memory_space=pltpu.VMEM)] * (inputs - scalars)
    return pl.pallas_call(
        kernel,
        out_shape=[
            jax.ShapeDtypeStruct(shape, jnp.float32) if isinstance(shape, tuple) else shape
            for shape in outs
        ],
        scratch_shapes=[pltpu.VMEM(shape, jnp.float32) for shape in scratch],
        compiler_params=pltpu.CompilerParams(vmem_limit_bytes=vmem_limit),
        cost_estimate=pl.CostEstimate(flops=flops, bytes_accessed=4 << 20, transcendentals=0),
        **specs,
    )


def shards(offsets, velocities, chain_label, partners, anchored):
    _, slots, planes, rows, lanes = offsets.shape
    devices = lax.axis_size("slab") * lax.axis_size("sub")
    padded = 4 * slots
    flops = planes * 27 * slots * slots * rows * lanes * 30
    tiles = (rows, lanes)
    field = (planes, 3 * slots, *tiles)
    edge = (planes, padded, lanes)
    near = ((planes + 2) * 9, 3 * slots, *tiles)
    pairs = [
        jax.ShapeDtypeStruct(
            (planes * 27, slots * slots // 2, 2 * rows, lanes), jnp.bfloat16
        ),
        (planes, slots, *tiles),
    ]
    ids = corner_devices()
    flat = offsets.reshape(3 * slots, planes, *tiles)
    labels = chain_label.astype(jnp.float32)
    wide = jnp.concatenate([flat, labels], axis=0)
    start = halo(*call(prepare_kernel, [(planes, 4 * slots, *tiles), edge, edge])(wide))
    extra = jnp.concatenate(
        [
            velocities.reshape(3 * slots, planes, *tiles),
            partners.reshape(2 * slots, planes, *tiles).astype(jnp.float32),
            anchored.astype(jnp.float32),
        ],
        axis=0,
    )
    half_velocity, place, first, last, *pairs = call(
        verlet_kernel,
        [velocities.shape, field, edge, edge, *pairs],
        [((planes + 2) * 9, 4 * slots, *tiles)],
        flops,
    )(extra, *start)
    places = halo(place, first, last)
    moves = ()
    for descent in range(DESCENTS):
        final = descent + 1 == DESCENTS

        def kernel(*refs, moving=bool(moves), final=final):
            descent_kernel(slots, planes, rows, moving, final, *refs)

        outs = [field, (devices, lanes)] if final else [field, edge, edge, (devices, padded, lanes)]
        moved = [x.shape for x in places] if moves else []
        scratch = [near]
        if final:
            moved, scratch = moved[:1], scratch + moved[1:]
        operands = (ids, *pairs, *places, *moves)
        results = call(kernel, moved + outs, scratch, flops, 1, len(operands))(*operands)
        peaks = lax.all_to_all(results[-1], ("slab", "sub"), 0, 0, tiled=True)
        if final:
            place, force, _ = results
            break
        if moves:
            places, results = results[:5], results[5:]
        moves = (*near_halo(*results[:3]), peaks)
    positions, unit_force = call(finish_kernel, [offsets.shape, offsets.shape])(
        place, force, peaks
    )
    return (positions, half_velocity, unit_force)


def solution(mesh):
    return jax.shard_map(
        shards,
        mesh=mesh,
        in_specs=(
            P(None, None, "slab", "sub", None),
            P(None, None, "slab", "sub", None),
            P(None, "slab", "sub", None),
            P(None, None, "slab", "sub", None),
            P(None, "slab", "sub", None),
        ),
        out_specs=(
            P(None, None, "slab", "sub", None),
            P(None, None, "slab", "sub", None),
            P(None, None, "slab", "sub", None),
        ),
        check_vma=False,
    )
```

```python
import jax
import jax.numpy as jnp
from jax import lax
from jax.experimental import pallas as pl
from jax.experimental.pallas import tpu as pltpu
from jax.sharding import PartitionSpec as P

DESCENTS = 3

cell_width = 1.25
soft_floor = 0.64
bond_stiff = 100.0
fene_floor = 0.2
time_step = 0.01
half_step = 0.005
half_step_sq = 5e-05
step_length = 0.1
tiny_eps = 1e-06

force_scale = 48.0
bond_range_sq = 9.0
live_barrier = 0.5
dead_barrier = 4.0
bond_unit = -bond_stiff * bond_range_sq / force_scale
code_low, code_high = 16, 91

vmem_limit = 12 << 20


def row_select(tile, row, index):
    rows = lax.broadcasted_iota(jnp.int32, tile.shape, 0)
    return jnp.where(rows == index, jnp.broadcast_to(row, tile.shape), tile)


def spread(main, low, high, shift_y, shift_z, store):
    rows, lanes = main.shape
    for step_y in (-1, 0, 1):
        tile = main
        if step_y == -1:
            tile = row_select(pltpu.roll(main, 1, 0), low, 0)
        elif step_y == 1:
            tile = row_select(pltpu.roll(main, rows - 1, 0), high, rows - 1)
        if shift_y and step_y:
            tile = tile + step_y * cell_width
        for step_z in (-1, 0, 1):
            moved = tile
            if step_z == -1:
                moved = pltpu.roll(tile, 1, 1)
            elif step_z == 1:
                moved = pltpu.roll(tile, lanes - 1, 1)
            if shift_z and step_z:
                moved = moved + step_z * cell_width
            store((step_y + 1) * 3 + step_z + 1, moved)


class Field:
    def __init__(self, refs, planes, channels, rows):
        self.own, self.low, self.high, self.down, self.up = refs
        self.planes, self.channels, self.rows = planes, channels, rows

    def plane(self, plane, channel):
        rows = self.rows
        if 1 <= plane <= self.planes:
            return (
                self.own[plane - 1, channel],
                self.low[plane - 1, pl.ds(channel, 1)],
                self.high[plane - 1, pl.ds(channel, 1)],
            )
        edge = self.down if plane == 0 else self.up
        base = self.channels * rows
        half = (edge.shape[0] - base) // 2
        return (
            edge[pl.ds(channel * rows, rows)],
            edge[pl.ds(base + channel, 1)],
            edge[pl.ds(base + half + channel, 1)],
        )


def pair_terms(own, other, barrier):
    sep = [a - b for a, b in zip(own, other)]
    dist_sq = sep[0] * sep[0] + sep[1] * sep[1] + sep[2] * sep[2]
    inv = 1.0 / jnp.maximum(dist_sq, soft_floor)
    inv_two = inv * inv
    coef = (inv_two * inv_two) * jnp.maximum(inv_two * inv - barrier, 0.0)
    return sep, dist_sq, coef


def bond_coef(dist_sq, strength):
    return strength * (1.0 / jnp.maximum(bond_range_sq - dist_sq, bond_range_sq * fene_floor))


def bond_cells(slots):
    return code_low // slots, code_high // slots + 1


def cell_runs(slots):
    bond_from, bond_to = bond_cells(slots)
    marks = sorted({0, 9, 18, 27, bond_from, bond_to})
    return [(a, b, a >= bond_from and b <= bond_to) for a, b in zip(marks, marks[1:])]


def plan(slots, planes):
    counts, runs = {"own": 0, "edge": 0}, []
    for plane in range(planes):
        for first, last, bonded in cell_runs(slots):
            part = "own" if 0 <= plane + first // 9 - 1 < planes else "edge"
            runs.append((plane, first, last, bonded, part, counts[part]))
            counts[part] += last - first
    return runs, counts


def sweep(slots, planes, parts, start, own_tile, near, body):
    totals = []
    for plane in range(planes):
        own = [own_tile(plane, c) for c in range(3 * slots)]
        if start is None:
            acc = [jnp.zeros_like(own[0]) for _ in range(3 * slots)]
        else:
            acc = [start[plane, c] for c in range(3 * slots)]
        for at_plane, first, last, bonded, part, base in plan(slots, planes)[0]:
            if at_plane != plane or part not in parts:
                continue
            step_x = first // 9 - 1
            moved = [own[s] - step_x * cell_width for s in range(slots)] + own[slots:]

            def step(cell, acc, moved=moved, bonded=bonded, plane=plane, part=part, base=base - first):
                acc = list(acc)
                for s2 in range(slots):
                    other = [near[plane * 9 + cell, c * slots + s2] for c in range(3)]
                    each = body(part, base + cell, plane, cell, s2, other, bonded)
                    for s1 in range(slots):
                        coef, sep = each(s1, [moved[c * slots + s1] for c in range(3)])
                        for c in range(3):
                            acc[c * slots + s1] = acc[c * slots + s1] + coef * sep[c]
                return tuple(acc)

            acc = lax.fori_loop(first, last, step, tuple(acc))
        totals.append(list(acc))
    return totals


def fill_near(field, near, planes, channels, slots):
    for plane in planes:
        for c in range(channels):

            def store(k, tile, plane=plane, c=c):
                near[plane * 9 + k, c] = tile

            main, lo, hi = field.plane(plane, c)
            spread(main, lo, hi, c // slots == 1, c // slots == 2, store)


def put_rows(low_ref, high_ref, plane, channel, tile):
    rows = tile.shape[0]
    low_ref[plane, pl.ds(channel, 1)] = tile[0:1]
    high_ref[plane, pl.ds(channel, 1)] = tile[rows - 1 : rows]


def prepare_kernel(wide_ref, field_ref, low_ref, high_ref):
    channels, planes, _, _ = wide_ref.shape
    for plane in range(planes):
        for c in range(channels):
            tile = wide_ref[c, plane]
            field_ref[plane, c] = tile
            put_rows(low_ref, high_ref, plane, c, tile)


def verlet_sums(slots, planes, part, start, extra_ref, own, barrier_ref, near):
    partner_at = 3 * slots

    def body(part, at, plane, cell, s2, other, bonded):
        label = near[plane * 9 + cell, 3 * slots + s2]
        alive = jnp.where(label < 0.0, dead_barrier, live_barrier)
        pending = []

        def each(s1, mine):
            sep, dist_sq, coef = pair_terms(mine, other, alive)
            barrier = jnp.where(label == own[plane, 3 * slots + s1], dead_barrier, alive)
            if bonded:
                code = (cell * slots + s2).astype(jnp.float32)
                strength = jnp.where(extra_ref[partner_at + s1, plane] == code, bond_unit, 0.0)
                strength += jnp.where(extra_ref[partner_at + slots + s1, plane] == code, bond_unit, 0.0)
                barrier = jnp.where(strength < 0.0, dead_barrier - strength, barrier)
                coef += bond_coef(dist_sq, strength)
            pending.append(barrier)
            if len(pending) == 2:
                both = jnp.concatenate(pending, axis=0).astype(barrier_ref.dtype)
                barrier_ref[at, (s2 * slots + s1) // 2] = both
                pending.clear()
            return coef, sep

        return each

    return sweep(slots, planes, (part,), start, lambda plane, c: own[plane, c], near, body)


def verlet_own_kernel(extra_ref, own, low, high, sum_ref, barrier_ref, near):
    planes, channels, rows, _ = own.shape
    slots = channels // 4
    field = Field((own, low, high, None, None), planes, channels, rows)
    fill_near(field, near, range(1, planes + 1), channels, slots)
    totals = verlet_sums(slots, planes, "own", None, extra_ref, own, barrier_ref, near)
    for plane in range(planes):
        for c in range(3 * slots):
            sum_ref[plane, c] = totals[plane][c]


def verlet_edge_kernel(
    extra_ref, own, down, up, sum_ref,
    half_ref, next_ref, next_low, next_high, barrier_ref, weight_ref, near,
):
    planes, channels, rows, _ = own.shape
    slots = channels // 4
    vel_at, anchor_at = 0, 5 * slots
    field = Field((own, None, None, down, up), planes, channels, rows)
    fill_near(field, near, (0, planes + 1), channels, slots)
    totals = verlet_sums(slots, planes, "edge", sum_ref, extra_ref, own, barrier_ref, near)
    for plane in range(planes):
        for s in range(slots):
            free = ((own[plane, 3 * slots + s] >= 0.0) & (extra_ref[anchor_at + s, plane] == 0.0)).astype(jnp.float32)
            weight_ref[plane, s] = free * force_scale
            for c in range(s, 3 * slots, slots):
                force = totals[plane][c] * (free * force_scale)
                moving = free * extra_ref[vel_at + c, plane]
                half_ref[c // slots, s, plane] = moving + half_step * force
                place = own[plane, c] + (time_step * moving + half_step_sq * force)
                next_ref[plane, c] = place
                put_rows(next_low, next_high, plane, c, place)


def descent_sums(slots, planes, parts, start, barriers, own, near):
    def body(part, at, plane, cell, s2, other, bonded):
        rows = other[0].shape[0]
        both = [
            barriers[part][at, (s2 * slots) // 2 + i].astype(jnp.float32) for i in range(slots // 2)
        ]

        def each(s1, mine):
            barrier = both[s1 // 2][(s1 % 2) * rows : (s1 % 2 + 1) * rows]
            sep, dist_sq, coef = pair_terms(mine, other, barrier)
            if bonded:
                coef += bond_coef(dist_sq, jnp.minimum(dead_barrier - barrier, 0.0))
            return coef, sep

        return each

    return sweep(slots, planes, parts, start, lambda plane, c: own[plane, c], near, body)


def descent_own_kernel(barrier_ref, own, low, high, sum_ref, near):
    planes, channels, rows, _ = own.shape
    slots = channels // 3
    field = Field((own, low, high, None, None), planes, channels, rows)
    fill_near(field, near, range(1, planes + 1), channels, slots)
    totals = descent_sums(slots, planes, ("own",), None, {"own": barrier_ref}, own, near)
    for plane in range(planes):
        for c in range(channels):
            sum_ref[plane, c] = totals[plane][c]


def inverse_peak(peaks):
    peak_force = jnp.sqrt(jnp.max(jnp.max(peaks, axis=0, keepdims=True), axis=1, keepdims=True))
    return 1.0 / (peak_force + tiny_eps)


def descent_kernel(slots, planes, rows, moves, last, *refs):
    refs = list(refs)

    def take(count):
        taken = refs[:count]
        del refs[:count]
        return taken

    ids, own_barrier, edge_barrier, weight_ref = take(4)
    barriers = {"own": own_barrier, "edge": edge_barrier}
    places = take(5)
    if not moves:
        (start,) = take(1)
        parts, fill_planes = ("edge",), (0, planes + 1)
    else:
        start, parts, fill_planes = None, ("own", "edge"), range(planes + 2)
        own, low, high, down, up, mixed = take(6)
        now = take(1) + refs[-4:] if last else take(5)
        if last:
            del refs[-4:]
        scale = step_length * inverse_peak(mixed[:, mixed.shape[1] - 1, :])
        for i, by in enumerate((own, low, high)):
            now[i][...] = places[i][...] + scale.reshape((1,) * len(by.shape)) * by[...]
        for i, by, corners in ((3, down, (3, 2)), (4, up, (1, 0))):
            base, pad = by.shape[0], mixed.shape[1]
            now[i][pl.ds(0, base)] = places[i][pl.ds(0, base)] + scale * by[...]
            for side, corner in enumerate(corners):
                at = pl.ds(base + side * pad, pad)
                now[i][at] = places[i][at] + scale * mixed[ids[corner]]
        places = now
    field = Field(places, planes, 3 * slots, rows)
    if last:
        force_ref, peak_ref, near = refs
    else:
        force_ref, force_low, force_high, mix_ref, near = refs
    fill_near(field, near, fill_planes, 3 * slots, slots)
    totals = descent_sums(slots, planes, parts, start, barriers, field.own, near)
    peak = None
    for plane in range(planes):
        forces = [total * weight_ref[plane, c % slots] for c, total in enumerate(totals[plane])]
        for c in range(3 * slots):
            force_ref[plane, c] = forces[c]
            if not last:
                put_rows(force_low, force_high, plane, c, forces[c])
        for s in range(slots):
            size = sum(forces[c * slots + s] * forces[c * slots + s] for c in range(3))
            peak = size if peak is None else jnp.maximum(peak, size)
    peak = jnp.max(peak, axis=0, keepdims=True)
    if last:
        peak_ref[...] = jnp.broadcast_to(peak, peak_ref.shape)
        return

    def fill(device, carry):
        mix_ref[device] = jnp.broadcast_to(peak, mix_ref.shape[1:])
        return carry

    lax.fori_loop(0, mix_ref.shape[0], fill, 0)
    for corner in range(4):
        plane = planes - 1 if corner < 2 else 0
        rows_ref = force_high if corner % 2 == 0 else force_low
        mix_ref[ids[corner], pl.ds(0, 3 * slots)] = rows_ref[plane, pl.ds(0, 3 * slots)]


def finish_kernel(place_ref, force_ref, peaks_ref, pos_ref, unit_ref):
    slots, planes = pos_ref.shape[1], pos_ref.shape[2]
    inverse = inverse_peak(peaks_ref[...])
    scale = step_length * inverse
    for plane in range(planes):
        for c in range(3 * slots):
            force = force_ref[plane, c]
            unit_ref[c // slots, c % slots, plane] = inverse * force
            pos_ref[c // slots, c % slots, plane] = place_ref[plane, c] + scale * force


def ring(axis):
    count = lax.axis_size(axis)
    forward = [(i, (i + 1) % count) for i in range(count)]
    return forward, [(b, a) for a, b in forward]


def row_halo(first_rows, last_rows):
    forward, backward = ring("sub")
    return lax.ppermute(last_rows, "sub", forward), lax.ppermute(first_rows, "sub", backward)


def plane_halo(own, low, high):
    planes, channels, rows, lanes = own.shape

    def packed(plane):
        return jnp.concatenate(
            [own[plane].reshape(channels * rows, lanes), low[plane], high[plane]], axis=0
        )

    forward, backward = ring("slab")
    down = lax.ppermute(packed(planes - 1), "slab", forward)
    up = lax.ppermute(packed(0), "slab", backward)
    return down, up


def near_halo(own, first_rows, last_rows):
    planes, channels, rows, lanes = own.shape
    forward, backward = ring("sub")
    low = lax.ppermute(last_rows, "sub", forward)
    high = lax.ppermute(first_rows, "sub", backward)
    forward, backward = ring("slab")
    flat = (channels * rows, lanes)
    down = lax.ppermute(own[planes - 1].reshape(flat), "slab", forward)
    up = lax.ppermute(own[0].reshape(flat), "slab", backward)
    return (own, low, high, down, up)


def corner_devices():
    slabs, subs = lax.axis_size("slab"), lax.axis_size("sub")
    x, y = lax.axis_index("slab"), lax.axis_index("sub")
    return jnp.stack(
        [
            ((x + i + slabs) % slabs) * subs + (y + j + subs) % subs
            for i in (1, -1)
            for j in (1, -1)
        ]
    ).astype(jnp.int32)


def call(kernel, outs, scratch=(), flops=0, scalars=0, inputs=0):
    specs = {}
    if scalars:
        specs["in_specs"] = [pl.BlockSpec(memory_space=pltpu.SMEM)] * scalars
        specs["in_specs"] += [pl.BlockSpec(memory_space=pltpu.VMEM)] * (inputs - scalars)
    return pl.pallas_call(
        kernel,
        out_shape=[
            jax.ShapeDtypeStruct(shape, jnp.float32) if isinstance(shape, tuple) else shape
            for shape in outs
        ],
        scratch_shapes=[pltpu.VMEM(shape, jnp.float32) for shape in scratch],
        compiler_params=pltpu.CompilerParams(vmem_limit_bytes=vmem_limit),
        cost_estimate=pl.CostEstimate(flops=flops, bytes_accessed=4 << 20, transcendentals=0),
        **specs,
    )


def shards(offsets, velocities, chain_label, partners, anchored):
    _, slots, planes, rows, lanes = offsets.shape
    devices = lax.axis_size("slab") * lax.axis_size("sub")
    padded = 4 * slots
    flops = planes * 27 * slots * slots * rows * lanes * 30
    tiles = (rows, lanes)
    field = (planes, 3 * slots, *tiles)
    edge = (planes, padded, lanes)
    near = ((planes + 2) * 9, 3 * slots, *tiles)
    counts = plan(slots, planes)[1]
    barrier = {
        part: jax.ShapeDtypeStruct((count, slots * slots // 2, 2 * rows, lanes), jnp.bfloat16)
        for part, count in counts.items()
    }
    share = {part: flops * count // (27 * planes) for part, count in counts.items()}
    ids = corner_devices()
    flat = offsets.reshape(3 * slots, planes, *tiles)
    labels = chain_label.astype(jnp.float32)
    wide = jnp.concatenate([flat, labels], axis=0)
    wide, first, last = call(prepare_kernel, [(planes, 4 * slots, *tiles), edge, edge])(wide)
    extra = jnp.concatenate(
        [
            velocities.reshape(3 * slots, planes, *tiles),
            partners.reshape(2 * slots, planes, *tiles).astype(jnp.float32),
            anchored.astype(jnp.float32),
        ],
        axis=0,
    )
    near_wide = ((planes + 2) * 9, 4 * slots, *tiles)
    low, high = row_halo(first, last)
    sums, own_barrier = call(
        verlet_own_kernel, [field, barrier["own"]], [near_wide], share["own"]
    )(extra, wide, low, high)
    down, up = plane_halo(wide, low, high)
    half_velocity, place, first, last, edge_barrier, weight = call(
        verlet_edge_kernel,
        [velocities.shape, field, edge, edge, barrier["edge"], (planes, slots, *tiles)],
        [near_wide],
        share["edge"],
    )(extra, wide, down, up, sums)
    low, high = row_halo(first, last)
    (sums,) = call(descent_own_kernel, [field], [near], share["own"])(own_barrier, place, low, high)
    places = (place, low, high, *plane_halo(place, low, high))
    moves = ()
    for descent in range(DESCENTS):
        final = descent + 1 == DESCENTS

        def kernel(*refs, moving=bool(moves), final=final):
            descent_kernel(slots, planes, rows, moving, final, *refs)

        outs = [field, (devices, lanes)] if final else [field, edge, edge, (devices, padded, lanes)]
        moved = [x.shape for x in places] if moves else []
        scratch = [near]
        if final:
            moved, scratch = moved[:1], scratch + moved[1:]
        operands = (ids, own_barrier, edge_barrier, weight, *places, *(moves or (sums,)))
        results = call(kernel, moved + outs, scratch, flops, 1, len(operands))(*operands)
        peaks = lax.all_to_all(results[-1], ("slab", "sub"), 0, 0, tiled=True)
        if final:
            place, force, _ = results
            break
        if moves:
            places, results = results[:5], results[5:]
        moves = (*near_halo(*results[:3]), peaks)
    positions, unit_force = call(finish_kernel, [offsets.shape, offsets.shape])(
        place, force, peaks
    )
    return (positions, half_velocity, unit_force)


def solution(mesh):
    return jax.shard_map(
        shards,
        mesh=mesh,
        in_specs=(
            P(None, None, "slab", "sub", None),
            P(None, None, "slab", "sub", None),
            P(None, "slab", "sub", None),
            P(None, None, "slab", "sub", None),
            P(None, "slab", "sub", None),
        ),
        out_specs=(
            P(None, None, "slab", "sub", None),
            P(None, None, "slab", "sub", None),
            P(None, None, "slab", "sub", None),
        ),
        check_vma=False,
    )
```

```python
import jax
import jax.numpy as jnp
from jax import lax
from jax.experimental import pallas as pl
from jax.experimental.pallas import tpu as pltpu
from jax.sharding import PartitionSpec as P

DESCENTS = 3

cell_width = 1.25
soft_floor = 0.64
bond_stiff = 100.0
fene_floor = 0.2
time_step = 0.01
half_step = 0.005
half_step_sq = 5e-05
step_length = 0.1
tiny_eps = 1e-06

force_scale = 48.0
bond_range_sq = 9.0
live_barrier = 0.5
dead_barrier = 4.0
bond_unit = -bond_stiff * bond_range_sq / force_scale
code_low, code_high = 16, 91

vmem_limit = 12 << 20


def row_select(tile, row, index):
    rows = lax.broadcasted_iota(jnp.int32, tile.shape, 0)
    return jnp.where(rows == index, jnp.broadcast_to(row, tile.shape), tile)


def spread(main, low, high, shift_y, shift_z, store):
    rows, lanes = main.shape
    for step_y in (-1, 0, 1):
        tile = main
        if step_y == -1:
            tile = row_select(pltpu.roll(main, 1, 0), low, 0)
        elif step_y == 1:
            tile = row_select(pltpu.roll(main, rows - 1, 0), high, rows - 1)
        if shift_y and step_y:
            tile = tile + step_y * cell_width
        for step_z in (-1, 0, 1):
            moved = tile
            if step_z == -1:
                moved = pltpu.roll(tile, 1, 1)
            elif step_z == 1:
                moved = pltpu.roll(tile, lanes - 1, 1)
            if shift_z and step_z:
                moved = moved + step_z * cell_width
            store((step_y + 1) * 3 + step_z + 1, moved)


class Field:
    def __init__(self, refs, planes, channels, rows):
        self.own, self.low, self.high, self.down, self.up = refs
        self.planes, self.channels, self.rows = planes, channels, rows

    def plane(self, plane, channel):
        rows = self.rows
        if 1 <= plane <= self.planes:
            return (
                self.own[plane - 1, channel],
                self.low[plane - 1, pl.ds(channel, 1)],
                self.high[plane - 1, pl.ds(channel, 1)],
            )
        edge = self.down if plane == 0 else self.up
        base = self.channels * rows
        half = (edge.shape[0] - base) // 2
        return (
            edge[pl.ds(channel * rows, rows)],
            edge[pl.ds(base + channel, 1)],
            edge[pl.ds(base + half + channel, 1)],
        )


def pair_terms(own, other, barrier):
    sep = [a - b for a, b in zip(own, other)]
    dist_sq = sep[0] * sep[0] + sep[1] * sep[1] + sep[2] * sep[2]
    inv = 1.0 / jnp.maximum(dist_sq, soft_floor)
    inv_two = inv * inv
    coef = (inv_two * inv_two) * jnp.maximum(inv_two * inv - barrier, 0.0)
    return sep, dist_sq, coef


def bond_coef(dist_sq, strength):
    return strength * (1.0 / jnp.maximum(bond_range_sq - dist_sq, bond_range_sq * fene_floor))


def bond_cells(slots):
    return code_low // slots, code_high // slots + 1


def cell_runs(slots):
    bond_from, bond_to = bond_cells(slots)
    marks = sorted({0, 9, 18, 27, bond_from, bond_to})
    return [(a, b, a >= bond_from and b <= bond_to) for a, b in zip(marks, marks[1:])]


def plan(slots, planes):
    counts, runs = {"own": 0, "edge": 0}, []
    for plane in range(planes):
        for first, last, bonded in cell_runs(slots):
            part = "own" if 0 <= plane + first // 9 - 1 < planes else "edge"
            runs.append((plane, first, last, bonded, part, counts[part]))
            counts[part] += last - first
    return runs, counts


def sweep(slots, planes, parts, start, own_tile, near, body):
    totals = []
    for plane in range(planes):
        own = [own_tile(plane, c) for c in range(3 * slots)]
        if start is None:
            acc = [jnp.zeros_like(own[0]) for _ in range(3 * slots)]
        else:
            acc = [start[plane, c] for c in range(3 * slots)]
        for at_plane, first, last, bonded, part, base in plan(slots, planes)[0]:
            if at_plane != plane or part not in parts:
                continue
            step_x = first // 9 - 1
            moved = [own[s] - step_x * cell_width for s in range(slots)] + own[slots:]

            def step(cell, acc, moved=moved, bonded=bonded, plane=plane, part=part, base=base - first):
                acc = list(acc)
                for s2 in range(slots):
                    other = [near[plane * 9 + cell, c * slots + s2] for c in range(3)]
                    each = body(part, base + cell, plane, cell, s2, other, bonded)
                    for s1 in range(slots):
                        coef, sep = each(s1, [moved[c * slots + s1] for c in range(3)])
                        for c in range(3):
                            acc[c * slots + s1] = acc[c * slots + s1] + coef * sep[c]
                return tuple(acc)

            acc = lax.fori_loop(first, last, step, tuple(acc))
        totals.append(list(acc))
    return totals


def fill_near(field, near, planes, channels, slots):
    for plane in planes:
        for c in range(channels):

            def store(k, tile, plane=plane, c=c):
                near[plane * 9 + k, c] = tile

            main, lo, hi = field.plane(plane, c)
            spread(main, lo, hi, c // slots == 1, c // slots == 2, store)


def put_rows(low_ref, high_ref, plane, channel, tile):
    rows = tile.shape[0]
    low_ref[plane, pl.ds(channel, 1)] = tile[0:1]
    high_ref[plane, pl.ds(channel, 1)] = tile[rows - 1 : rows]


def prepare_kernel(wide_ref, field_ref, low_ref, high_ref):
    channels, planes, _, _ = wide_ref.shape
    for plane in range(planes):
        for c in range(channels):
            tile = wide_ref[c, plane]
            field_ref[plane, c] = tile
            put_rows(low_ref, high_ref, plane, c, tile)


def verlet_sums(slots, planes, part, start, extra_ref, own, barrier_ref, near):
    partner_at = 3 * slots

    def body(part, at, plane, cell, s2, other, bonded):
        label = near[plane * 9 + cell, 3 * slots + s2]
        alive = jnp.where(label < 0.0, dead_barrier, live_barrier)
        pending = []

        def each(s1, mine):
            sep, dist_sq, coef = pair_terms(mine, other, alive)
            barrier = jnp.where(label == own[plane, 3 * slots + s1], dead_barrier, alive)
            if bonded:
                code = (cell * slots + s2).astype(jnp.float32)
                strength = jnp.where(extra_ref[partner_at + s1, plane] == code, bond_unit, 0.0)
                strength += jnp.where(extra_ref[partner_at + slots + s1, plane] == code, bond_unit, 0.0)
                barrier = jnp.where(strength < 0.0, dead_barrier - strength, barrier)
                coef += bond_coef(dist_sq, strength)
            pending.append(barrier)
            if len(pending) == 2:
                both = jnp.concatenate(pending, axis=0).astype(barrier_ref.dtype)
                barrier_ref[at, (s2 * slots + s1) // 2] = both
                pending.clear()
            return coef, sep

        return each

    return sweep(slots, planes, (part,), start, lambda plane, c: own[plane, c], near, body)


def verlet_own_kernel(extra_ref, own, low, high, sum_ref, barrier_ref, near):
    planes, channels, rows, _ = own.shape
    slots = channels // 4
    field = Field((own, low, high, None, None), planes, channels, rows)
    fill_near(field, near, range(1, planes + 1), channels, slots)
    totals = verlet_sums(slots, planes, "own", None, extra_ref, own, barrier_ref, near)
    for plane in range(planes):
        for c in range(3 * slots):
            sum_ref[plane, c] = totals[plane][c]


def verlet_edge_kernel(
    extra_ref, own, down, up, sum_ref,
    half_ref, next_ref, next_low, next_high, barrier_ref, weight_ref, near,
):
    planes, channels, rows, _ = own.shape
    slots = channels // 4
    vel_at, anchor_at = 0, 5 * slots
    field = Field((own, None, None, down, up), planes, channels, rows)
    fill_near(field, near, (0, planes + 1), channels, slots)
    totals = verlet_sums(slots, planes, "edge", sum_ref, extra_ref, own, barrier_ref, near)
    for plane in range(planes):
        for s in range(slots):
            free = ((own[plane, 3 * slots + s] >= 0.0) & (extra_ref[anchor_at + s, plane] == 0.0)).astype(jnp.float32)
            weight_ref[plane, s] = free * force_scale
            for c in range(s, 3 * slots, slots):
                force = totals[plane][c] * (free * force_scale)
                moving = free * extra_ref[vel_at + c, plane]
                half_ref[c // slots, s, plane] = moving + half_step * force
                place = own[plane, c] + (time_step * moving + half_step_sq * force)
                next_ref[plane, c] = place
                put_rows(next_low, next_high, plane, c, place)


def descent_sums(slots, planes, parts, start, barriers, own, near):
    def body(part, at, plane, cell, s2, other, bonded):
        rows = other[0].shape[0]
        both = [
            barriers[part][at, (s2 * slots) // 2 + i].astype(jnp.float32) for i in range(slots // 2)
        ]

        def each(s1, mine):
            barrier = both[s1 // 2][(s1 % 2) * rows : (s1 % 2 + 1) * rows]
            sep, dist_sq, coef = pair_terms(mine, other, barrier)
            if bonded:
                coef += bond_coef(dist_sq, jnp.minimum(dead_barrier - barrier, 0.0))
            return coef, sep

        return each

    return sweep(slots, planes, parts, start, lambda plane, c: own[plane, c], near, body)


def descent_own_kernel(barrier_ref, own, low, high, sum_ref, near):
    planes, channels, rows, _ = own.shape
    slots = channels // 3
    field = Field((own, low, high, None, None), planes, channels, rows)
    fill_near(field, near, range(1, planes + 1), channels, slots)
    totals = descent_sums(slots, planes, ("own",), None, {"own": barrier_ref}, own, near)
    for plane in range(planes):
        for c in range(channels):
            sum_ref[plane, c] = totals[plane][c]


def inverse_peak(peaks):
    peak_force = jnp.sqrt(jnp.max(jnp.max(peaks, axis=0, keepdims=True), axis=1, keepdims=True))
    return 1.0 / (peak_force + tiny_eps)


def descent_kernel(slots, planes, rows, moves, last, *refs):
    refs = list(refs)

    def take(count):
        taken = refs[:count]
        del refs[:count]
        return taken

    ids, own_barrier, edge_barrier, weight_ref = take(4)
    barriers = {"own": own_barrier, "edge": edge_barrier}
    places = take(5)
    if not moves:
        (start,) = take(1)
        parts, fill_planes = ("edge",), (0, planes + 1)
    else:
        start, parts, fill_planes = None, ("own", "edge"), range(planes + 2)
        own, down, up, mixed = take(4)
        now = take(1) + refs[-4:] if last else take(5)
        if last:
            del refs[-4:]
        scale = step_length * inverse_peak(mixed[:, mixed.shape[1] - 1, :])
        now[0][...] = places[0][...] + scale.reshape((1, 1, 1, 1)) * own[...]
        pad = mixed.shape[1] // planes
        for i, side in ((1, 5), (2, 4)):
            for plane in range(planes):
                by = mixed[ids[side], pl.ds(plane * pad, pad)]
                now[i][plane] = places[i][plane] + scale * by
        for i, by, corners in ((3, down, (3, 2)), (4, up, (1, 0))):
            base = by.shape[0]
            now[i][pl.ds(0, base)] = places[i][pl.ds(0, base)] + scale * by[...]
            for side, corner in enumerate(corners):
                at = pl.ds(base + side * pad, pad)
                now[i][at] = places[i][at] + scale * mixed[ids[corner], pl.ds(0, pad)]
        places = now
    field = Field(places, planes, 3 * slots, rows)
    if last:
        force_ref, peak_ref, near = refs
    else:
        force_ref, mix_ref, near = refs
    fill_near(field, near, fill_planes, 3 * slots, slots)
    totals = descent_sums(slots, planes, parts, start, barriers, field.own, near)
    peak = None
    for plane in range(planes):
        forces = [total * weight_ref[plane, c % slots] for c, total in enumerate(totals[plane])]
        for c in range(3 * slots):
            force_ref[plane, c] = forces[c]
        for s in range(slots):
            size = sum(forces[c * slots + s] * forces[c * slots + s] for c in range(3))
            peak = size if peak is None else jnp.maximum(peak, size)
    peak = jnp.max(peak, axis=0, keepdims=True)
    if last:
        peak_ref[...] = jnp.broadcast_to(peak, peak_ref.shape)
        return

    def fill(device, carry):
        mix_ref[device] = jnp.broadcast_to(peak, mix_ref.shape[1:])
        return carry

    lax.fori_loop(0, mix_ref.shape[0], fill, 0)
    pad = mix_ref.shape[1] // planes
    for side in range(6):
        step_y = 1 if side % 2 == 0 else -1
        sent = range(planes) if side >= 4 else (planes - 1 if side < 2 else 0,)
        for at, plane in enumerate(sent):
            for c in range(3 * slots):
                row = rows - 1 if step_y == 1 else 0
                mix_ref[ids[side], pl.ds(at * pad + c, 1)] = force_ref[plane, c, pl.ds(row, 1)]


def finish_kernel(place_ref, force_ref, peaks_ref, pos_ref, unit_ref):
    slots, planes = pos_ref.shape[1], pos_ref.shape[2]
    inverse = inverse_peak(peaks_ref[...])
    scale = step_length * inverse
    for plane in range(planes):
        for c in range(3 * slots):
            force = force_ref[plane, c]
            unit_ref[c // slots, c % slots, plane] = inverse * force
            pos_ref[c // slots, c % slots, plane] = place_ref[plane, c] + scale * force


def ring(axis):
    count = lax.axis_size(axis)
    forward = [(i, (i + 1) % count) for i in range(count)]
    return forward, [(b, a) for a, b in forward]


def row_halo(first_rows, last_rows):
    forward, backward = ring("sub")
    return lax.ppermute(last_rows, "sub", forward), lax.ppermute(first_rows, "sub", backward)


def plane_halo(own, low, high):
    planes, channels, rows, lanes = own.shape

    def packed(plane):
        return jnp.concatenate(
            [own[plane].reshape(channels * rows, lanes), low[plane], high[plane]], axis=0
        )

    forward, backward = ring("slab")
    down = lax.ppermute(packed(planes - 1), "slab", forward)
    up = lax.ppermute(packed(0), "slab", backward)
    return down, up


def near_planes(own):
    planes, channels, rows, lanes = own.shape
    forward, backward = ring("slab")
    flat = (channels * rows, lanes)
    down = lax.ppermute(own[planes - 1].reshape(flat), "slab", forward)
    up = lax.ppermute(own[0].reshape(flat), "slab", backward)
    return down, up


def side_devices():
    slabs, subs = lax.axis_size("slab"), lax.axis_size("sub")
    x, y = lax.axis_index("slab"), lax.axis_index("sub")
    return jnp.stack(
        [
            ((x + i + slabs) % slabs) * subs + (y + j + subs) % subs
            for i in (1, -1, 0)
            for j in (1, -1)
        ]
    ).astype(jnp.int32)


def call(kernel, outs, scratch=(), flops=0, scalars=0, inputs=0):
    specs = {}
    if scalars:
        specs["in_specs"] = [pl.BlockSpec(memory_space=pltpu.SMEM)] * scalars
        specs["in_specs"] += [pl.BlockSpec(memory_space=pltpu.VMEM)] * (inputs - scalars)
    return pl.pallas_call(
        kernel,
        out_shape=[
            jax.ShapeDtypeStruct(shape, jnp.float32) if isinstance(shape, tuple) else shape
            for shape in outs
        ],
        scratch_shapes=[pltpu.VMEM(shape, jnp.float32) for shape in scratch],
        compiler_params=pltpu.CompilerParams(vmem_limit_bytes=vmem_limit),
        cost_estimate=pl.CostEstimate(flops=flops, bytes_accessed=4 << 20, transcendentals=0),
        **specs,
    )


def shards(offsets, velocities, chain_label, partners, anchored):
    _, slots, planes, rows, lanes = offsets.shape
    devices = lax.axis_size("slab") * lax.axis_size("sub")
    padded = 4 * slots
    flops = planes * 27 * slots * slots * rows * lanes * 30
    tiles = (rows, lanes)
    field = (planes, 3 * slots, *tiles)
    edge = (planes, padded, lanes)
    near = ((planes + 2) * 9, 3 * slots, *tiles)
    counts = plan(slots, planes)[1]
    barrier = {
        part: jax.ShapeDtypeStruct((count, slots * slots // 2, 2 * rows, lanes), jnp.bfloat16)
        for part, count in counts.items()
    }
    share = {part: flops * count // (27 * planes) for part, count in counts.items()}
    ids = side_devices()
    flat = offsets.reshape(3 * slots, planes, *tiles)
    labels = chain_label.astype(jnp.float32)
    wide = jnp.concatenate([flat, labels], axis=0)
    wide, first, last = call(prepare_kernel, [(planes, 4 * slots, *tiles), edge, edge])(wide)
    extra = jnp.concatenate(
        [
            velocities.reshape(3 * slots, planes, *tiles),
            partners.reshape(2 * slots, planes, *tiles).astype(jnp.float32),
            anchored.astype(jnp.float32),
        ],
        axis=0,
    )
    near_wide = ((planes + 2) * 9, 4 * slots, *tiles)
    low, high = row_halo(first, last)
    sums, own_barrier = call(
        verlet_own_kernel, [field, barrier["own"]], [near_wide], share["own"]
    )(extra, wide, low, high)
    down, up = plane_halo(wide, low, high)
    half_velocity, place, first, last, edge_barrier, weight = call(
        verlet_edge_kernel,
        [velocities.shape, field, edge, edge, barrier["edge"], (planes, slots, *tiles)],
        [near_wide],
        share["edge"],
    )(extra, wide, down, up, sums)
    low, high = row_halo(first, last)
    (sums,) = call(descent_own_kernel, [field], [near], share["own"])(own_barrier, place, low, high)
    places = (place, low, high, *plane_halo(place, low, high))
    moves = ()
    for descent in range(DESCENTS):
        final = descent + 1 == DESCENTS

        def kernel(*refs, moving=bool(moves), final=final):
            descent_kernel(slots, planes, rows, moving, final, *refs)

        outs = [field, (devices, lanes)] if final else [field, (devices, planes * padded, lanes)]
        moved = [x.shape for x in places] if moves else []
        scratch = [near]
        if final:
            moved, scratch = moved[:1], scratch + moved[1:]
        operands = (ids, own_barrier, edge_barrier, weight, *places, *(moves or (sums,)))
        results = call(kernel, moved + outs, scratch, flops, 1, len(operands))(*operands)
        peaks = lax.all_to_all(results[-1], ("slab", "sub"), 0, 0, tiled=True)
        if final:
            place, force, _ = results
            break
        if moves:
            places, results = results[:5], results[5:]
        moves = (results[0], *near_planes(results[0]), peaks)
    positions, unit_force = call(finish_kernel, [offsets.shape, offsets.shape])(
        place, force, peaks
    )
    return (positions, half_velocity, unit_force)


def solution(mesh):
    return jax.shard_map(
        shards,
        mesh=mesh,
        in_specs=(
            P(None, None, "slab", "sub", None),
            P(None, None, "slab", "sub", None),
            P(None, "slab", "sub", None),
            P(None, None, "slab", "sub", None),
            P(None, "slab", "sub", None),
        ),
        out_specs=(
            P(None, None, "slab", "sub", None),
            P(None, None, "slab", "sub", None),
            P(None, None, "slab", "sub", None),
        ),
        check_vma=False,
    )
```
